512 devices in a mesh: ctx: 64 (over z_hi, y, core), exp: 8 (over x, z_lo).
Axes of the slice: x: 4, y: 8, z: 8 (z_hi: 4, z_lo: 2; z = z_hi * 2 + z_lo), core: 2. Of those that a mesh axis runs over, the one named last changes fastest.
Arguments:
- queries: bfloat16 [4096, 16, 128], P(('exp', 'ctx')), may hold values from -6 to 6
- key_heads: bfloat16 [4096, 8, 128], P('ctx', 'exp'), may hold values from -6 to 6
- value_heads: bfloat16 [4096, 8, 128], P('ctx', 'exp'), may hold values from -6 to 6
- expert_ids: int32 [4096, 16], P(('exp', 'ctx')), may hold values from 0 to 63, all different within a row; in each aligned block of 8 rows (0 to 7, 8 to 15, ...) at most 3 rows name the same one
- gate_logits: float32 [4096, 16], P(('exp', 'ctx')), may hold values from -4 to 4
- out_weight: bfloat16 [64, 128, 8192], P('exp', None, 'ctx'), may hold values from -0.5 to 0.5
Outputs:
- mixed_out: bfloat16 [4096, 8192], P('exp', 'ctx')
The draws below stay inside these ranges and needn't reach their ends.
Inputs may be any that keep to these rules, and one draw needn't show every extreme that they name: `expert_ids`: each token names 16 different experts; among the 8 tokens of an aligned block no expert is named by more than 3 tokens, a bound that some block reaches.
All inputs are finite; a program needn't handle non-finite values.
Results may differ from the reference program's by a relative error of at most 0.018.
Values may be sent and summed in bfloat16 or wider, within the bound.
No kernel may reach another device: no remote copies, remote signals or barrier semaphores. Data moves between devices by JAX's collectives and lax.ppermute only.
A program may use at most 64 MiB of HBM per device.

```python
import math
import jax
import jax.numpy as jnp
import numpy as np
from jax import lax

D = 8192
EXPERTS = 64
KVH = 8
HD = 128
TOP = 16
TOK_DEV = 8
MOST = 3
TOKENS = 4096
N_EXP = 8


def draw_queries(key, part):
    drawn = jnp.clip(1.5 * jax.random.normal(jax.random.fold_in(key, 21), (TOKENS, TOP, HD), jnp.float32), -6.0, 6.0)
    return drawn.astype(jnp.bfloat16)


def draw_key_heads(key, part):
    drawn = jnp.clip(jax.random.normal(jax.random.fold_in(key, 22), (TOKENS, KVH, HD), jnp.float32), -6.0, 6.0)
    return drawn.astype(jnp.bfloat16)


def steps_of(key, shape, split, least, high):
    level = 1.0
    for axis_at, blocks in split:
        draws = jax.random.uniform(jax.random.fold_in(jax.random.fold_in(key, 6), axis_at), (blocks,), jnp.float32, least / len(split), high / len(split))
        level = level * jnp.repeat(jnp.exp(draws), shape[axis_at] // blocks).reshape((-1,) + (1,) * (len(shape) - 1 - axis_at))
    return level


def routed_block(stream_key, own, number, rows, amount, top, bound, skew):
    ranking = jax.random.permutation(stream_key, amount)
    heavy_load, usual = shares(amount, rows * top, bound, skew, True), shares(amount, rows * top, bound, skew, False)
    places = jnp.arange(amount)

    def named(tallies, turn):
        used = int((tallies > 0).sum())
        fixed = max(1, used // 4)
        passed = fixed + (places - fixed + turn * (used - fixed)) % max(1, amount - fixed)
        return jnp.zeros((amount,), jnp.int32).at[ranking[jnp.where(places < fixed, places, passed)]].set(jnp.asarray(tallies, jnp.int32))

    tallies = jnp.where(number % 4 == 0, named(heavy_load, number // 4), named(usual, number - number // 4 - 1))
    mixed = jax.random.permutation(jax.random.fold_in(own, 3), amount)
    donor, taker = mixed[0:amount // 2 * 2:2], mixed[1:amount // 2 * 2:2]
    slack = jnp.minimum(tallies[donor] - 1, bound - tallies[taker]) // 2
    slack = jnp.where((donor == ranking[0]) | (taker == ranking[0]) | (tallies[taker] == 0), 0, jnp.maximum(slack, 0))
    passed = jax.random.randint(jax.random.fold_in(own, 4), (amount // 2,), 0, 1 << 20) % (slack + 1)
    tallies = tallies.at[donor].add(-passed).at[taker].add(passed)
    members = jnp.searchsorted(jnp.cumsum(tallies), jnp.arange(rows * top), side="right").astype(jnp.int32)
    listing = members.reshape(top, rows).T
    listing = listing[jax.random.permutation(jax.random.fold_in(own, 1), rows)]
    turn = jax.random.randint(jax.random.fold_in(own, 2), (rows, 1), 0, top)
    return jnp.take_along_axis(listing, (jnp.arange(top)[None, :] + turn) % top, axis=1)


def shares(amount, total, reach, slope, full):
    weights = [(1 << 20) // math.isqrt(standing ** slope) + 1 for standing in range(1, amount + 1)]
    largest = reach if full else min(reach, max(-(-total // amount), total * weights[0] // sum(weights)))
    least = 1 if total - largest >= amount - 1 else 0
    given, surplus = [largest] + [least] * (amount - 1), total - largest - least * (amount - 1)
    while surplus > 0:
        movable = [i for i in range(1, amount) if given[i] < largest] or [i for i in range(1, amount) if given[i] < reach]
        whole, remaining = sum([weights[i] for i in movable]), surplus
        for i in movable:
            extra = min(reach - given[i], max(1, remaining * weights[i] // whole), surplus)
            given[i] = given[i] + extra
            surplus = surplus - extra
    return np.array(given)


def bell_draw(own_key, extent, scale, reach, split=(), kind=jnp.bfloat16):
    values = scale * jax.random.normal(own_key, extent, jnp.float32)
    if split:
        values = values * steps_of(own_key, extent, split, -0.22, 0.18)
    return jnp.clip(values, -reach, reach).astype(kind)


def setup_inputs(seed: int = 0) -> dict:
    streams_of = jax.random.split(jax.random.key(seed), 7)
    queries = draw_queries(jax.random.fold_in(streams_of[6], 71), 0)
    key_heads = draw_key_heads(jax.random.fold_in(streams_of[6], 71), 0)
    value_heads = bell_draw(streams_of[2], (TOKENS, KVH, HD), 1.0, 6.0, ((0, 64), (1, 8)))
    expert_ids_keys = jax.random.split(jax.random.fold_in(streams_of[3], 1), TOKENS // TOK_DEV)
    expert_ids_turns = jax.random.permutation(jax.random.fold_in(streams_of[3], 3), TOKENS // TOK_DEV)
    expert_ids = jax.vmap(lambda own, number: routed_block(jax.random.fold_in(streams_of[3], 2), own, number, TOK_DEV, EXPERTS, TOP, MOST, 2))(expert_ids_keys, expert_ids_turns).reshape((TOKENS, TOP))
    gate_logits = jnp.clip(jax.random.uniform(streams_of[4], (TOKENS, TOP), jnp.float32, -4.0, 4.0) * steps_of(streams_of[4], (TOKENS, TOP), ((0, 512),), -0.4, 0.0), -4.0, 4.0)
    out_weight = bell_draw(streams_of[5], (EXPERTS, HD, D), HD ** -0.5, 0.5, ((0, 8), (2, 64)))
    return dict(queries=queries, key_heads=key_heads, value_heads=value_heads, expert_ids=expert_ids, gate_logits=gate_logits, out_weight=out_weight)


NEG_FLOOR = -1e30


def reference(queries, key_heads, value_heads, expert_ids, gate_logits, out_weight):
    gate_exp = jnp.exp(gate_logits)
    gate_values = (gate_exp / jnp.sum(gate_exp, axis=1, keepdims=True)).astype(jnp.bfloat16)
    group_size = EXPERTS // KVH
    head_of = expert_ids // group_size
    block_tokens = 128
    key_pos = jnp.arange(TOKENS, dtype=jnp.int32)

    def one_head(head_num, collected):
        head_keys = lax.dynamic_index_in_dim(key_heads, head_num, 1, keepdims=False)
        head_values = lax.dynamic_index_in_dim(value_heads, head_num, 1, keepdims=False)

        def one_block(block_num):
            block_queries = lax.dynamic_slice_in_dim(queries, block_num * block_tokens, block_tokens, 0)
            block_queries = block_queries.reshape(block_tokens * TOP, HD)
            query_pos = block_num * block_tokens + jnp.arange(block_tokens * TOP, dtype=jnp.int32) // TOP
            scores = jnp.dot(block_queries, head_keys.T, preferred_element_type=jnp.float32) * (HD ** -0.5)
            visible = key_pos[None, :] <= query_pos[:, None]
            scores = jnp.where(visible, scores, NEG_FLOOR)
            row_max = jnp.max(scores, axis=1, keepdims=True)
            exponents = jnp.where(visible, jnp.exp(scores - row_max), 0.0)
            weighted = jnp.dot(exponents.astype(jnp.bfloat16), head_values, preferred_element_type=jnp.float32)
            normed = weighted / jnp.sum(exponents, axis=1, keepdims=True)
            return normed.reshape(block_tokens, TOP, HD)

        head_out = lax.map(one_block, jnp.arange(TOKENS // block_tokens, dtype=jnp.int32))
        head_out = head_out.reshape(TOKENS, TOP, HD)
        return collected + jnp.where((head_of == head_num)[:, :, None], head_out, 0.0)

    attended = lax.fori_loop(0, KVH, one_head, jnp.zeros((TOKENS, TOP, HD), jnp.float32))
    gated_rows = (gate_values.astype(jnp.float32)[:, :, None] * attended).astype(jnp.bfloat16)
    per_device = EXPERTS // N_EXP

    def one_group(group_num, accumulated):
        def one_expert(local_num, partial_value):
            expert_num = group_num * per_device + local_num
            chosen = jnp.sum(jnp.where((expert_ids == expert_num)[:, :, None], gated_rows.astype(jnp.float32), 0.0), axis=1)
            chosen = chosen.astype(jnp.bfloat16)
            weight_now = lax.dynamic_index_in_dim(out_weight, expert_num, 0, keepdims=False)
            return partial_value + jnp.dot(chosen, weight_now, preferred_element_type=jnp.float32)

        partial_value = lax.fori_loop(0, per_device, one_expert, jnp.zeros((TOKENS, D), jnp.float32))
        rounded = lax.optimization_barrier(partial_value.astype(jnp.bfloat16))
        return accumulated + rounded.astype(jnp.float32)

    accumulated = lax.fori_loop(0, N_EXP, one_group, jnp.zeros((TOKENS, D), jnp.float32))
    return accumulated.astype(jnp.bfloat16)
```

```python
import math

import jax
import jax.numpy as jnp
from jax import lax
from jax.experimental import pallas as pl
from jax.experimental.pallas import tpu as pltpu
from jax.sharding import Mesh, PartitionSpec as P

EXPERTS = 64
HD = 128
TOP = 16
MOST = 3
TOK = 8
ROWS = TOK * TOP
GROUPS = 8
PER = EXPERTS // GROUPS
SLOTS = 32
SPAN = 64
CHIPS = 32
KVROWS = 2 * SPAN + 8
NEG_FLOOR = -1e30


f32 = jnp.float32
bf16 = jnp.bfloat16
NT = (((1,), (1,)), ((), ()))


def iota(shape, dim):
    return lax.broadcasted_iota(jnp.int32, shape, dim)


def prep_kernel(q_ref, k_ref, v_ref, ids_ref, logit_ref, qsend_ref, kvsend_ref, back_ref):
    spread = (iota((TOP, ROWS), 1) % TOP == iota((TOP, ROWS), 0)).astype(f32)
    own = iota((TOK, ROWS), 1) // TOP == iota((TOK, ROWS), 0)

    def as_row(table):
        wide = jnp.dot(table, spread, precision=lax.Precision.HIGHEST, preferred_element_type=f32)
        return jnp.sum(jnp.where(own, wide, 0.0), axis=0, keepdims=True)

    id_row = as_row(ids_ref[...].astype(f32))
    gate_exp = jnp.exp(logit_ref[...])
    gate_row = as_row(gate_exp / jnp.sum(gate_exp, axis=1, keepdims=True))
    id_int = id_row.astype(jnp.int32)
    id_col = jnp.broadcast_to(id_row, (ROWS, ROWS)).T
    earlier = (id_col == id_row) & (iota((ROWS, ROWS), 0) < iota((ROWS, ROWS), 1))
    rank = jnp.sum(earlier.astype(f32), axis=0, keepdims=True).astype(jnp.int32)
    slot = (id_int // PER) * SLOTS + (id_int % PER) * MOST + rank
    placed = (iota((GROUPS * SLOTS, ROWS), 0) == slot).astype(bf16)
    rows = jnp.dot(placed, q_ref[...], preferred_element_type=f32)
    tag_at = iota((8, ROWS), 0)
    tags = jnp.where(tag_at == 0, (iota((8, ROWS), 1) // TOP).astype(f32), 0.0)
    tags = jnp.where(tag_at == 1, gate_row, tags).astype(bf16)
    for g in range(GROUPS):
        here = (iota((ROWS, ROWS), 0) == slot - g * SLOTS).astype(bf16)
        info = lax.dot_general(tags, here, NT, preferred_element_type=f32)
        qsend_ref[g] = jnp.concatenate(
            [rows[g * SLOTS : g * SLOTS + PER * MOST], info], axis=0
        ).astype(bf16)
    slot_col = jnp.broadcast_to(slot.astype(f32), (ROWS, ROWS)).T.astype(jnp.int32)
    lane = iota((ROWS, ROWS), 1)
    back_ref[:, :ROWS] = (lane == slot_col).astype(bf16)
    back_ref[:, ROWS:] = (lane + ROWS == slot_col).astype(bf16)
    keys = k_ref[...]
    values = v_ref[...]
    ids = jnp.broadcast_to(id_row, (8, ROWS)).astype(bf16)

    def fill(i, _):
        kvsend_ref[i, 0:SPAN] = keys
        kvsend_ref[i, SPAN : 2 * SPAN] = values
        kvsend_ref[i, 2 * SPAN : KVROWS] = ids
        return 0

    lax.fori_loop(0, CHIPS, fill, 0)


def attend_kernel(at_ref, q_ref, kva_ref, kvb_ref, out_ref, s_ref):
    n = GROUPS * SLOTS
    step = 4
    width = step * SPAN
    steps = CHIPS // step
    queries = q_ref[...].reshape(n, HD)
    ctx = at_ref[0]
    core = at_ref[1]
    tags = jnp.concatenate(
        [q_ref[g, PER * MOST : SLOTS].astype(f32) for g in range(GROUPS)], axis=0
    )
    tags = jnp.concatenate([tags, tags], axis=0).T[0:SLOTS]
    token = jnp.concatenate([tags[:, g * 8 : g * 8 + 1] for g in range(GROUPS)], axis=0)
    gate = jnp.concatenate([tags[:, g * 8 + 1 : g * 8 + 2] for g in range(GROUPS)], axis=0)
    source = iota((n, 1), 0) // SLOTS
    pos = (source * (2 * CHIPS) + ctx) * TOK + token.astype(jnp.int32)
    scale = HD ** (-0.5) * math.log2(math.e)
    lane = iota((1, width), 1)

    def score(i, best, kv_ref, parity, base):
        keys = kv_ref[pl.ds(i * step, step), 0:SPAN, :].reshape(width, HD)
        scores = lax.dot_general(queries, keys, NT, preferred_element_type=f32) * scale
        key_pos = (2 * (i * step + lane // SPAN) + parity) * SPAN + lane % SPAN
        scores = jnp.where(key_pos <= pos, scores, NEG_FLOOR)
        s_ref[base + i] = scores
        return jnp.maximum(best, jnp.maximum(scores[:, :HD], scores[:, HD:]))

    def score_both(i, best):
        best = score(i, best, kva_ref, core, 0)
        return score(i, best, kvb_ref, 1 - core, steps)

    best = lax.fori_loop(0, steps, score_both, jnp.full((n, HD), NEG_FLOOR, f32))
    best = jnp.max(best, axis=1, keepdims=True)

    def weigh(i, carried, kv_ref, base):
        total, acc = carried
        exps = jnp.exp2(s_ref[base + i] - best)
        values = kv_ref[pl.ds(i * step, step), SPAN : 2 * SPAN, :].reshape(width, HD)
        acc = acc + jnp.dot(exps.astype(bf16), values, preferred_element_type=f32)
        return total + exps[:, :HD] + exps[:, HD:], acc

    def weigh_both(i, carried):
        return weigh(i, weigh(i, carried, kva_ref, 0), kvb_ref, steps)

    zero = jnp.zeros((n, HD), f32)
    total, acc = lax.fori_loop(0, steps, weigh_both, (zero, zero))
    total = jnp.sum(total, axis=1, keepdims=True)
    out_ref[...] = (gate * (acc / total)).astype(bf16).reshape(GROUPS, SLOTS, HD)


def compact_kernel(back_ref, got_ref, out_ref):
    rows = jnp.dot(
        back_ref[...], got_ref[...].reshape(GROUPS * SLOTS, HD), preferred_element_type=f32
    ).astype(bf16)

    def fill(i, _):
        out_ref[i] = rows
        return 0

    lax.fori_loop(0, CHIPS, fill, 0)


def project_kernel(at_ref, rows_ref, kv_ref, wa_ref, wb_ref, mine_ref, other_ref, a_ref):
    x = at_ref[2]
    zl = at_ref[3]
    token = iota((1, ROWS), 1) // TOP
    target_at = iota((EXPERTS * TOK, ROWS), 0)

    def spread(i):
        ids = kv_ref[i, 2 * SPAN : KVROWS, :].astype(f32)[0:1].astype(jnp.int32)
        group = ids // PER
        piece = ((x - group // 2 + 4) % 4) * 2 + (group % 2 + zl) % 2
        expert = piece * PER + ids % PER
        target = (expert % 2) * (EXPERTS // 2 * TOK) + (expert // 2) * TOK + token
        hot = (target_at == target).astype(bf16)
        got = jnp.dot(hot, rows_ref[i], preferred_element_type=f32)
        return got.reshape(EXPERTS, TOK, HD)

    def fill(i, _):
        both = jnp.concatenate([spread(2 * i), spread(2 * i + 1)], axis=1).astype(bf16)
        at = pl.ds(pl.multiple_of(i * 2 * TOK, 2 * TOK), 2 * TOK)
        a_ref[:, at, 0:HD] = both[: EXPERTS // 2]
        a_ref[:, at, HD : 2 * HD] = both[EXPERTS // 2 :]
        return 0

    lax.fori_loop(0, CHIPS // 2, fill, 0)

    def add(p, acc):
        wa = wa_ref[pl.ds(2 * p, 2)].reshape(2 * HD, HD)
        wb = wb_ref[pl.ds(2 * p, 2)].reshape(2 * HD, HD)
        weight = jnp.concatenate([wa, wb], axis=1)
        return acc + jnp.dot(a_ref[p], weight, preferred_element_type=f32)

    n = CHIPS * TOK
    acc = lax.fori_loop(0, EXPERTS // 2, add, jnp.zeros((n, 2 * HD), f32))
    mine_ref[...] = acc[:, :HD].astype(bf16)
    other_ref[...] = acc[:, HD:].astype(bf16)


SMEM = pl.BlockSpec(memory_space=pltpu.SMEM)
VMEM = pl.BlockSpec(memory_space=pltpu.VMEM)


def shifted(x, axis, count, by):
    return lax.ppermute(x, axis, [(i, (i + by) % count) for i in range(count)])


def body(queries, key_heads, value_heads, expert_ids, gate_logits, out_weight):
    zh, y, core = lax.axis_index("zh"), lax.axis_index("y"), lax.axis_index("core")
    x, zl = lax.axis_index("x"), lax.axis_index("zl")
    ctx = (zh * 8 + y) * 2 + core
    at = jnp.stack([ctx, core, x, zl]).astype(jnp.int32)
    shape = jax.ShapeDtypeStruct
    qsend, kvsend, back = pl.pallas_call(
        prep_kernel,
        in_specs=[VMEM] * 5,
        out_specs=[VMEM] * 3,
        out_shape=[
            shape((GROUPS, SLOTS, HD), bf16),
            shape((CHIPS, KVROWS, HD), bf16),
            shape((ROWS, GROUPS * SLOTS), bf16),
        ],
        name="prep",
    )(
        queries.reshape(ROWS, HD),
        key_heads.reshape(SPAN, HD),
        value_heads.reshape(SPAN, HD),
        expert_ids,
        gate_logits,
    )
    pair = jnp.concatenate([out_weight, shifted(out_weight, "zl", 2, 1)], axis=0)
    pieces = jnp.concatenate([pair] + [shifted(pair, "x", 4, k) for k in range(1, 4)], axis=0)
    pieces_other = shifted(pieces, "core", 2, 1)

    qgot = lax.all_to_all(qsend, ("x", "zl"), 0, 0, tiled=True)
    kva = lax.all_to_all(kvsend, ("zh", "y"), 0, 0, tiled=True)
    kvb = shifted(kva, "core", 2, 1)
    attended = pl.pallas_call(
        attend_kernel,
        in_specs=[SMEM, VMEM, VMEM, VMEM],
        out_specs=VMEM,
        out_shape=shape((GROUPS, SLOTS, HD), bf16),
        scratch_shapes=[pltpu.VMEM((16, GROUPS * SLOTS, 4 * SPAN), f32)],
        name="attend",
    )(at, qgot, kva, kvb)
    home = lax.all_to_all(attended, ("x", "zl"), 0, 0, tiled=True)
    rows = pl.pallas_call(
        compact_kernel,
        in_specs=[VMEM, VMEM],
        out_specs=VMEM,
        out_shape=shape((CHIPS, ROWS, HD), bf16),
        name="compact",
    )(back, home)
    rows = lax.all_to_all(rows, ("zh", "y"), 0, 0, tiled=True)
    mine, other = pl.pallas_call(
        project_kernel,
        in_specs=[SMEM, VMEM, VMEM, VMEM, VMEM],
        out_specs=[VMEM, VMEM],
        out_shape=[shape((CHIPS * TOK, HD), bf16)] * 2,
        scratch_shapes=[pltpu.VMEM((EXPERTS // 2, CHIPS * TOK, 2 * HD), bf16)],
        name="project",
    )(at, rows, kva, pieces, pieces_other)
    got = shifted(other, "core", 2, 1)
    mine = mine.reshape(CHIPS, 1, TOK, HD)
    got = got.reshape(CHIPS, 1, TOK, HD)
    first = jnp.where(core == 0, mine, got)
    second = jnp.where(core == 0, got, mine)
    return jnp.concatenate([first, second], axis=1).reshape(2 * CHIPS * TOK, HD)


def solution(mesh):
    fine = Mesh(mesh.devices.reshape(4, 8, 2, 4, 2), ("zh", "y", "core", "x", "zl"))
    ctx, exp = ("zh", "y", "core"), ("x", "zl")
    in_specs = (
        P(exp + ctx, None, None),
        P(ctx, exp, None),
        P(ctx, exp, None),
        P(exp + ctx, None),
        P(exp + ctx, None),
        P(exp, None, ctx),
    )
    return jax.shard_map(body, mesh=fine, in_specs=in_specs, out_specs=P(exp, ctx), check_vma=False)
```

```python
import math

import jax
import jax.numpy as jnp
from jax import lax
from jax.experimental import pallas as pl
from jax.experimental.pallas import tpu as pltpu
from jax.sharding import Mesh, PartitionSpec as P


EXPERTS = 64
HD = 128
TOP = 16
MOST = 3
TOK = 8
ROWS = TOK * TOP
GROUPS = 8
PER = EXPERTS // GROUPS
SLOTS = 32
SPAN = 64
CHIPS = 32
KVROWS = 2 * SPAN + 8
NEG_FLOOR = -1e30


f32 = jnp.float32
bf16 = jnp.bfloat16
NT = (((1,), (1,)), ((), ()))


def iota(shape, dim):
    return lax.broadcasted_iota(jnp.int32, shape, dim)


def prep_kernel(q_ref, k_ref, v_ref, ids_ref, logit_ref, qsend_ref, kvsend_ref, back_ref):
    spread = (iota((TOP, ROWS), 1) % TOP == iota((TOP, ROWS), 0)).astype(f32)
    own = iota((TOK, ROWS), 1) // TOP == iota((TOK, ROWS), 0)

    def as_row(table):
        wide = jnp.dot(table, spread, precision=lax.Precision.HIGHEST, preferred_element_type=f32)
        return jnp.sum(jnp.where(own, wide, 0.0), axis=0, keepdims=True)

    id_row = as_row(ids_ref[...].astype(f32))
    gate_exp = jnp.exp(logit_ref[...])
    gate_row = as_row(gate_exp / jnp.sum(gate_exp, axis=1, keepdims=True))
    id_int = id_row.astype(jnp.int32)
    id_col = jnp.broadcast_to(id_row, (ROWS, ROWS)).T
    earlier = (id_col == id_row) & (iota((ROWS, ROWS), 0) < iota((ROWS, ROWS), 1))
    rank = jnp.sum(earlier.astype(f32), axis=0, keepdims=True).astype(jnp.int32)
    slot = (id_int // PER) * SLOTS + (id_int % PER) * MOST + rank
    placed = (iota((GROUPS * SLOTS, ROWS), 0) == slot).astype(bf16)
    rows = jnp.dot(placed, q_ref[...], preferred_element_type=f32)
    tag_at = iota((8, ROWS), 0)
    tags = jnp.where(tag_at == 0, (iota((8, ROWS), 1) // TOP).astype(f32), 0.0)
    tags = jnp.where(tag_at == 1, gate_row, tags).astype(bf16)
    for g in range(GROUPS):
        here = (iota((ROWS, ROWS), 0) == slot - g * SLOTS).astype(bf16)
        info = lax.dot_general(tags, here, NT, preferred_element_type=f32)
        qsend_ref[g] = jnp.concatenate(
            [rows[g * SLOTS : g * SLOTS + PER * MOST], info], axis=0
        ).astype(bf16)
    slot_col = jnp.broadcast_to(slot.astype(f32), (ROWS, ROWS)).T.astype(jnp.int32)
    lane = iota((ROWS, ROWS), 1)
    back_ref[:, :ROWS] = (lane == slot_col).astype(bf16)
    back_ref[:, ROWS:] = (lane + ROWS == slot_col).astype(bf16)
    keys = k_ref[...]
    values = v_ref[...]
    ids = jnp.broadcast_to(id_row, (8, ROWS)).astype(bf16)

    def fill(i, _):
        kvsend_ref[i, 0:SPAN] = keys
        kvsend_ref[i, SPAN : 2 * SPAN] = values
        kvsend_ref[i, 2 * SPAN : KVROWS] = ids
        return 0

    lax.fori_loop(0, CHIPS, fill, 0)


def attend_kernel(at_ref, q_ref, kva_ref, kvb_ref, out_ref, s_ref):
    n = GROUPS * SLOTS
    step = 4
    width = step * SPAN
    steps = CHIPS // step
    queries = q_ref[...].reshape(n, HD)
    ctx = at_ref[0]
    core = at_ref[1]
    tags = jnp.concatenate(
        [q_ref[g, PER * MOST : SLOTS].astype(f32) for g in range(GROUPS)], axis=0
    )
    tags = jnp.concatenate([tags, tags], axis=0).T[0:SLOTS]
    token = jnp.concatenate([tags[:, g * 8 : g * 8 + 1] for g in range(GROUPS)], axis=0)
    gate = jnp.concatenate([tags[:, g * 8 + 1 : g * 8 + 2] for g in range(GROUPS)], axis=0)
    source = iota((n, 1), 0) // SLOTS
    pos = (source * (2 * CHIPS) + ctx) * TOK + token.astype(jnp.int32)
    scale = HD ** (-0.5) * math.log2(math.e)
    lane = iota((1, width), 1)

    def score(i, best, kv_ref, parity, base):
        keys = kv_ref[pl.ds(i * step, step), 0:SPAN, :].reshape(width, HD)
        scores = lax.dot_general(queries, keys, NT, preferred_element_type=f32) * scale
        key_pos = (2 * (i * step + lane // SPAN) + parity) * SPAN + lane % SPAN
        scores = jnp.where(key_pos <= pos, scores, NEG_FLOOR)
        s_ref[base + i] = scores
        return jnp.maximum(best, jnp.maximum(scores[:, :HD], scores[:, HD:]))

    def score_both(i, best):
        best = score(i, best, kva_ref, core, 0)
        return score(i, best, kvb_ref, 1 - core, steps)

    best = lax.fori_loop(0, steps, score_both, jnp.full((n, HD), NEG_FLOOR, f32))
    best = jnp.max(best, axis=1, keepdims=True)

    def weigh(i, carried, kv_ref, base):
        total, acc = carried
        exps = jnp.exp2(s_ref[base + i] - best)
        values = kv_ref[pl.ds(i * step, step), SPAN : 2 * SPAN, :].reshape(width, HD)
        acc = acc + jnp.dot(exps.astype(bf16), values, preferred_element_type=f32)
        return total + exps[:, :HD] + exps[:, HD:], acc

    def weigh_both(i, carried):
        return weigh(i, weigh(i, carried, kva_ref, 0), kvb_ref, steps)

    zero = jnp.zeros((n, HD), f32)
    total, acc = lax.fori_loop(0, steps, weigh_both, (zero, zero))
    total = jnp.sum(total, axis=1, keepdims=True)
    out_ref[...] = (gate * (acc / total)).astype(bf16).reshape(GROUPS, SLOTS, HD)


def compact_kernel(back_ref, got_ref, out_ref):
    rows = jnp.dot(
        back_ref[...], got_ref[...].reshape(GROUPS * SLOTS, HD), preferred_element_type=f32
    ).astype(bf16)

    def fill(i, _):
        out_ref[i] = rows
        return 0

    lax.fori_loop(0, CHIPS, fill, 0)


def project_kernel(at_ref, rows_ref, kv_ref, *refs):
    w_refs = refs[:8]
    mine_ref, other_ref, a_ref = refs[8:]
    x = at_ref[0]
    zl = at_ref[1]
    token = iota((1, ROWS), 1) // TOP
    target_at = iota((EXPERTS * TOK, ROWS), 0)

    def spread(i):
        ids = kv_ref[i, 2 * SPAN : KVROWS, :].astype(f32)[0:1].astype(jnp.int32)
        group = ids // PER
        piece = ((x - group // 2 + 4) % 4) * 2 + (group % 2 + zl) % 2
        target = (piece * PER + ids % PER) * TOK + token
        hot = (target_at == target).astype(bf16)
        got = jnp.dot(hot, rows_ref[i], preferred_element_type=f32)
        return got.reshape(EXPERTS, TOK, HD)

    def fill(i, _):
        both = jnp.concatenate([spread(2 * i), spread(2 * i + 1)], axis=1).astype(bf16)
        at = pl.ds(pl.multiple_of(i * 2 * TOK, 2 * TOK), 2 * TOK)
        for e in range(EXPERTS):
            a_ref[e // PER, at, (e % PER) * HD : (e % PER + 1) * HD] = both[e]
        return 0

    lax.fori_loop(0, CHIPS // 2, fill, 0)

    def product(half):
        total = None
        for piece in range(GROUPS):
            ref = w_refs[4 * half + piece // 2]
            weight = ref[piece % 2 * PER : (piece % 2 + 1) * PER].reshape(PER * HD, HD)
            term = jnp.dot(a_ref[piece], weight, preferred_element_type=f32)
            total = term if total is None else total + term
        return total

    mine_ref[...] = product(0).astype(bf16)
    other_ref[...] = product(1).astype(bf16)


SMEM = pl.BlockSpec(memory_space=pltpu.SMEM)
VMEM = pl.BlockSpec(memory_space=pltpu.VMEM)


def shifted(x, axis, count, by):
    return lax.ppermute(x, axis, [(i, (i + by) % count) for i in range(count)])


def run(queries, key_heads, value_heads, expert_ids, gate_logits, out_weight):
    zh, y, core = lax.axis_index("zh"), lax.axis_index("y"), lax.axis_index("core")
    x, zl = lax.axis_index("x"), lax.axis_index("zl")
    ctx = (zh * 8 + y) * 2 + core
    at = jnp.stack([ctx, core]).astype(jnp.int32)
    at_exp = jnp.stack([x, zl, core]).astype(jnp.int32)
    shape = jax.ShapeDtypeStruct
    qsend, kvsend, back = pl.pallas_call(
        prep_kernel,
        in_specs=[VMEM] * 5,
        out_specs=[VMEM] * 3,
        out_shape=[
            shape((GROUPS, SLOTS, HD), bf16),
            shape((CHIPS, KVROWS, HD), bf16),
            shape((ROWS, GROUPS * SLOTS), bf16),
        ],
        name="prep",
    )(
        queries.reshape(ROWS, HD),
        key_heads.reshape(SPAN, HD),
        value_heads.reshape(SPAN, HD),
        expert_ids,
        gate_logits,
    )
    qgot = lax.all_to_all(qsend, ("x", "zl"), 0, 0, tiled=True)
    kva = lax.all_to_all(kvsend, ("zh", "y"), 0, 0, tiled=True)
    near = shifted(out_weight, "zl", 2, 1)
    pair = jnp.concatenate([out_weight, near], axis=0)
    pieces = [pair]
    for k in range(1, 4):
        pieces.append(shifted(pair, "x", 4, k))
    far = []
    for k in range(4):
        far.append(shifted(pieces[k], "core", 2, 1))
    kvb = shifted(kva, "core", 2, 1)
    attended = pl.pallas_call(
        attend_kernel,
        in_specs=[SMEM, VMEM, VMEM, VMEM],
        out_specs=VMEM,
        out_shape=shape((GROUPS, SLOTS, HD), bf16),
        scratch_shapes=[pltpu.VMEM((16, GROUPS * SLOTS, 4 * SPAN), f32)],
        name="attend",
    )(at, qgot, kva, kvb)
    home = lax.all_to_all(attended, ("x", "zl"), 0, 0, tiled=True)
    rows = pl.pallas_call(
        compact_kernel,
        in_specs=[VMEM, VMEM],
        out_specs=VMEM,
        out_shape=shape((CHIPS, ROWS, HD), bf16),
        name="compact",
    )(back, home)
    rows = lax.all_to_all(rows, ("zh", "y"), 0, 0, tiled=True)
    mine, other = pl.pallas_call(
        project_kernel,
        in_specs=[SMEM] + [VMEM] * 10,
        out_specs=[VMEM, VMEM],
        out_shape=[shape((CHIPS * TOK, HD), bf16)] * 2,
        scratch_shapes=[pltpu.VMEM((GROUPS, CHIPS * TOK, PER * HD), bf16)],
        name="project",
    )(at_exp, rows, kva, *pieces, *far)
    got = shifted(other, "core", 2, 1)
    mine = mine.reshape(CHIPS, 1, TOK, HD)
    got = got.reshape(CHIPS, 1, TOK, HD)
    first = jnp.where(core == 0, mine, got)
    second = jnp.where(core == 0, got, mine)
    return jnp.concatenate([first, second], axis=1).reshape(2 * CHIPS * TOK, HD)


def solution(mesh):
    fine = Mesh(mesh.devices.reshape(4, 8, 2, 4, 2), ("zh", "y", "core", "x", "zl"))
    ctx, exp = ("zh", "y", "core"), ("x", "zl")
    in_specs = (
        P(exp + ctx, None, None),
        P(ctx, exp, None),
        P(ctx, exp, None),
        P(exp + ctx, None),
        P(exp + ctx, None),
        P(exp, None, ctx),
    )
    return jax.shard_map(run, mesh=fine, in_specs=in_specs, out_specs=P(exp, ctx), check_vma=False)
```

```python
import math

import jax
import jax.numpy as jnp
from jax import lax
from jax.experimental import pallas as pl
from jax.experimental.pallas import tpu as pltpu
from jax.sharding import Mesh, PartitionSpec as P


EXPERTS = 64
HD = 128
TOP = 16
MOST = 3
TOK = 8
ROWS = TOK * TOP
GROUPS = 8
PER = EXPERTS // GROUPS
SLOTS = 32
SPAN = 64
CHIPS = 32
KVROWS = 2 * SPAN + 8
NEG_FLOOR = -1e30


f32 = jnp.float32
bf16 = jnp.bfloat16
NT = (((1,), (1,)), ((), ()))


def iota(shape, dim):
    return lax.broadcasted_iota(jnp.int32, shape, dim)


def away(group, x, zl):
    return ((group // 2 - x + 4) % 4) * 2 + (group % 2 + zl) % 2


def prep_kernel(q_ref, k_ref, v_ref, ids_ref, logit_ref, kvsend_ref, back_ref, *qsend_refs):
    x = lax.axis_index("x")
    zl = lax.axis_index("zl")
    spread = (iota((TOP, ROWS), 1) % TOP == iota((TOP, ROWS), 0)).astype(f32)
    own = iota((TOK, ROWS), 1) // TOP == iota((TOK, ROWS), 0)

    def as_row(table):
        wide = jnp.dot(table, spread, precision=lax.Precision.HIGHEST, preferred_element_type=f32)
        return jnp.sum(jnp.where(own, wide, 0.0), axis=0, keepdims=True)

    id_row = as_row(ids_ref[...].astype(f32))
    gate_exp = jnp.exp(logit_ref[...])
    gate_row = as_row(gate_exp / jnp.sum(gate_exp, axis=1, keepdims=True))
    id_int = id_row.astype(jnp.int32)
    id_col = jnp.broadcast_to(id_row, (ROWS, ROWS)).T
    earlier = (id_col == id_row) & (iota((ROWS, ROWS), 0) < iota((ROWS, ROWS), 1))
    rank = jnp.sum(earlier.astype(f32), axis=0, keepdims=True).astype(jnp.int32)
    group = id_int // PER
    within = (id_int % PER) * MOST + rank
    slot = away(group, x, zl) * SLOTS + within
    placed = (iota((GROUPS * SLOTS, ROWS), 0) == slot).astype(bf16)
    rows = jnp.dot(placed, q_ref[...], preferred_element_type=f32)
    tag_at = iota((8, ROWS), 0)
    tags = jnp.where(tag_at == 0, (iota((8, ROWS), 1) // TOP).astype(f32), 0.0)
    tags = jnp.where(tag_at == 1, gate_row, tags).astype(bf16)
    for g in range(GROUPS):
        here = (iota((ROWS, ROWS), 0) == slot - g * SLOTS).astype(bf16)
        info = lax.dot_general(tags, here, NT, preferred_element_type=f32)
        qsend_refs[g][...] = jnp.concatenate(
            [rows[g * SLOTS : g * SLOTS + PER * MOST], info], axis=0
        ).astype(bf16)
    slot = group * SLOTS + within
    slot_col = jnp.broadcast_to(slot.astype(f32), (ROWS, ROWS)).T.astype(jnp.int32)
    lane = iota((ROWS, ROWS), 1)
    back_ref[:, :ROWS] = (lane == slot_col).astype(bf16)
    back_ref[:, ROWS:] = (lane + ROWS == slot_col).astype(bf16)
    keys = k_ref[...]
    values = v_ref[...]
    ids = jnp.broadcast_to(id_row, (8, ROWS)).astype(bf16)

    def fill(i, _):
        kvsend_ref[i, 0:SPAN] = keys
        kvsend_ref[i, SPAN : 2 * SPAN] = values
        kvsend_ref[i, 2 * SPAN : KVROWS] = ids
        return 0

    lax.fori_loop(0, CHIPS, fill, 0)


def attend_kernel(at_ref, kva_ref, kvb_ref, *refs):
    q_refs, (out_ref, s_ref) = refs[:GROUPS], refs[GROUPS:]
    n = GROUPS * SLOTS
    step = 4
    width = step * SPAN
    steps = CHIPS // step
    queries = jnp.concatenate([q_ref[...] for q_ref in q_refs], axis=0)
    ctx = at_ref[0]
    core = at_ref[1]
    tags = jnp.concatenate(
        [q_ref[PER * MOST : SLOTS].astype(f32) for q_ref in q_refs], axis=0
    )
    tags = jnp.concatenate([tags, tags], axis=0).T[0:SLOTS]
    token = jnp.concatenate([tags[:, g * 8 : g * 8 + 1] for g in range(GROUPS)], axis=0)
    gate = jnp.concatenate([tags[:, g * 8 + 1 : g * 8 + 2] for g in range(GROUPS)], axis=0)
    sources = [
        ((at_ref[2] - d // 2 + 4) % 4) * 2 + (at_ref[3] + d % 2) % 2 for d in range(GROUPS)
    ]
    source = jnp.concatenate([jnp.full((SLOTS, 1), d, jnp.int32) for d in sources], axis=0)
    pos = (source * (2 * CHIPS) + ctx) * TOK + token.astype(jnp.int32)
    scale = HD ** (-0.5) * math.log2(math.e)
    lane = iota((1, width), 1)

    def score(i, best, kv_ref, parity, base):
        keys = kv_ref[pl.ds(i * step, step), 0:SPAN, :].reshape(width, HD)
        scores = lax.dot_general(queries, keys, NT, preferred_element_type=f32) * scale
        key_pos = (2 * (i * step + lane // SPAN) + parity) * SPAN + lane % SPAN
        scores = jnp.where(key_pos <= pos, scores, NEG_FLOOR)
        s_ref[base + i] = scores
        return jnp.maximum(best, jnp.maximum(scores[:, :HD], scores[:, HD:]))

    def score_both(i, best):
        best = score(i, best, kva_ref, core, 0)
        return score(i, best, kvb_ref, 1 - core, steps)

    best = lax.fori_loop(0, steps, score_both, jnp.full((n, HD), NEG_FLOOR, f32))
    best = jnp.max(best, axis=1, keepdims=True)

    def weigh(i, carried, kv_ref, base):
        total, acc = carried
        exps = jnp.exp2(s_ref[base + i] - best)
        values = kv_ref[pl.ds(i * step, step), SPAN : 2 * SPAN, :].reshape(width, HD)
        acc = acc + jnp.dot(exps.astype(bf16), values, preferred_element_type=f32)
        return total + exps[:, :HD] + exps[:, HD:], acc

    def weigh_both(i, carried):
        return weigh(i, weigh(i, carried, kva_ref, 0), kvb_ref, steps)

    zero = jnp.zeros((n, HD), f32)
    total, acc = lax.fori_loop(0, steps, weigh_both, (zero, zero))
    total = jnp.sum(total, axis=1, keepdims=True)
    result = (gate * (acc / total)).astype(bf16)
    for d in range(GROUPS):
        out_ref[sources[d]] = result[d * SLOTS : (d + 1) * SLOTS]


def compact_kernel(back_ref, got_ref, out_ref):
    rows = jnp.dot(
        back_ref[...], got_ref[...].reshape(GROUPS * SLOTS, HD), preferred_element_type=f32
    ).astype(bf16)

    def fill(i, _):
        out_ref[i] = rows
        return 0

    lax.fori_loop(0, CHIPS, fill, 0)


def project_kernel(at_ref, rows_ref, kv_ref, *refs):
    near_refs, far_refs = refs[:4], refs[4:8]
    mine_ref, other_ref, a_ref, far_ref, sems = refs[8:]
    copies = [
        pltpu.make_async_copy(far_refs[k], far_ref.at[k], sems.at[k]) for k in range(4)
    ]
    for copy in copies:
        copy.start()
    x = at_ref[0]
    zl = at_ref[1]
    token = iota((1, ROWS), 1) // TOP
    target_at = iota((EXPERTS * TOK, ROWS), 0)

    def spread(i):
        ids = kv_ref[i, 2 * SPAN : KVROWS, :].astype(f32)[0:1].astype(jnp.int32)
        group = ids // PER
        piece = ((x - group // 2 + 4) % 4) * 2 + (group % 2 + zl) % 2
        target = (piece * PER + ids % PER) * TOK + token
        hot = (target_at == target).astype(bf16)
        got = jnp.dot(hot, rows_ref[i], preferred_element_type=f32)
        return got.reshape(EXPERTS, TOK, HD)

    def fill(i, _):
        both = jnp.concatenate([spread(2 * i), spread(2 * i + 1)], axis=1).astype(bf16)
        at = pl.ds(pl.multiple_of(i * 2 * TOK, 2 * TOK), 2 * TOK)
        for e in range(EXPERTS):
            a_ref[e // PER, at, (e % PER) * HD : (e % PER + 1) * HD] = both[e]
        return 0

    lax.fori_loop(0, CHIPS // 2, fill, 0)

    for copy in copies:
        copy.wait()
    total = jnp.zeros((CHIPS * TOK, 2 * HD), f32)
    for piece in range(GROUPS):
        part = slice(piece % 2 * PER, (piece % 2 + 1) * PER)
        near = near_refs[piece // 2][part].reshape(PER * HD, HD)
        far = far_ref[piece // 2, part].reshape(PER * HD, HD)
        weight = jnp.concatenate([near, far], axis=1)
        total = total + jnp.dot(a_ref[piece], weight, preferred_element_type=f32)
    mine_ref[...] = total[:, :HD].astype(bf16)
    other_ref[...] = total[:, HD:].astype(bf16)


SMEM = pl.BlockSpec(memory_space=pltpu.SMEM)
VMEM = pl.BlockSpec(memory_space=pltpu.VMEM)
ANY = pl.BlockSpec(memory_space=pl.ANY)


def shifted(x, axis, count, by):
    return lax.ppermute(x, axis, [(i, (i + by) % count) for i in range(count)])


def run(queries, key_heads, value_heads, expert_ids, gate_logits, out_weight):
    zh, y, core = lax.axis_index("zh"), lax.axis_index("y"), lax.axis_index("core")
    x, zl = lax.axis_index("x"), lax.axis_index("zl")
    ctx = (zh * 8 + y) * 2 + core
    at = jnp.stack([ctx, core, x, zl]).astype(jnp.int32)
    at_exp = jnp.stack([x, zl, core]).astype(jnp.int32)
    shape = jax.ShapeDtypeStruct
    kvsend, back, *qsend = pl.pallas_call(
        prep_kernel,
        in_specs=[VMEM] * 5,
        out_specs=[VMEM] * 10,
        out_shape=[
            shape((CHIPS, KVROWS, HD), bf16),
            shape((ROWS, GROUPS * SLOTS), bf16),
        ]
        + [shape((SLOTS, HD), bf16)] * GROUPS,
        compiler_params=pltpu.CompilerParams(vmem_limit_bytes=8 << 20),
        name="prep",
    )(
        queries.reshape(ROWS, HD),
        key_heads.reshape(SPAN, HD),
        value_heads.reshape(SPAN, HD),
        expert_ids,
        gate_logits,
    )
    qgot = [qsend[0]]
    for d in range(1, GROUPS):
        moves = [
            (i, (i // 2 + d // 2) % 4 * 2 + (i + d) % 2) for i in range(GROUPS)
        ]
        qgot.append(lax.ppermute(qsend[d], ("x", "zl"), moves))
    kva = lax.all_to_all(kvsend, ("zh", "y"), 0, 0, tiled=True)
    near = shifted(out_weight, "zl", 2, 1)
    pair = jnp.concatenate([out_weight, near], axis=0)
    pieces = [pair]
    for k in range(1, 4):
        pieces.append(shifted(pair, "x", 4, k))
    far = []
    for k in range(4):
        far.append(shifted(pieces[k], "core", 2, 1))
    kvb = shifted(kva, "core", 2, 1)
    attended = pl.pallas_call(
        attend_kernel,
        in_specs=[SMEM] + [VMEM] * 10,
        out_specs=VMEM,
        out_shape=shape((GROUPS, SLOTS, HD), bf16),
        scratch_shapes=[pltpu.VMEM((16, GROUPS * SLOTS, 4 * SPAN), f32)],
        compiler_params=pltpu.CompilerParams(vmem_limit_bytes=14 << 20),
        name="attend",
    )(at, kva, kvb, *qgot)
    home = lax.all_to_all(attended, ("x", "zl"), 0, 0, tiled=True)
    rows = pl.pallas_call(
        compact_kernel,
        in_specs=[VMEM, VMEM],
        out_specs=VMEM,
        out_shape=shape((CHIPS, ROWS, HD), bf16),
        compiler_params=pltpu.CompilerParams(vmem_limit_bytes=8 << 20),
        name="compact",
    )(back, home)
    rows = lax.all_to_all(rows, ("zh", "y"), 0, 0, tiled=True)
    mine, other = pl.pallas_call(
        project_kernel,
        in_specs=[SMEM] + [VMEM] * 6 + [ANY] * 4,
        out_specs=[VMEM, VMEM],
        out_shape=[shape((CHIPS * TOK, HD), bf16)] * 2,
        scratch_shapes=[
            pltpu.VMEM((GROUPS, CHIPS * TOK, PER * HD), bf16),
            pltpu.VMEM((4, 2 * PER, HD, HD), bf16),
            pltpu.SemaphoreType.DMA((4,)),
        ],
        compiler_params=pltpu.CompilerParams(vmem_limit_bytes=20 << 20),
        name="project",
    )(at_exp, rows, kva, *pieces, *far)
    got = shifted(other, "core", 2, 1)
    own = lax.broadcasted_iota(jnp.int32, (CHIPS, 2, TOK, HD), 1) == core
    mine = mine.reshape(CHIPS, 1, TOK, HD)
    got = got.reshape(CHIPS, 1, TOK, HD)
    return jnp.where(own, mine, got).reshape(2 * CHIPS * TOK, HD)


def solution(mesh):
    fine = Mesh(mesh.devices.reshape(4, 8, 2, 4, 2), ("zh", "y", "core", "x", "zl"))
    ctx, exp = ("zh", "y", "core"), ("x", "zl")
    in_specs = (
        P(exp + ctx, None, None),
        P(ctx, exp, None),
        P(ctx, exp, None),
        P(exp + ctx, None),
        P(exp + ctx, None),
        P(exp, None, ctx),
    )
    return jax.shard_map(run, mesh=fine, in_specs=in_specs, out_specs=P(exp, ctx), check_vma=False)
```

```python
import math

import jax
import jax.numpy as jnp
from jax import lax
from jax.experimental import pallas as pl
from jax.experimental.pallas import tpu as pltpu
from jax.sharding import Mesh, PartitionSpec as P


EXPERTS = 64
HD = 128
TOP = 16
MOST = 3
TOK = 8
ROWS = TOK * TOP
GROUPS = 8
PER = EXPERTS // GROUPS
SLOTS = 32
SPAN = 64
CHIPS = 32
KVROWS = 2 * SPAN + 8
NEG_FLOOR = -1e30


f32 = jnp.float32
bf16 = jnp.bfloat16
NT = (((1,), (1,)), ((), ()))


def iota(shape, dim):
    return lax.broadcasted_iota(jnp.int32, shape, dim)


def away(group, x, zl):
    return ((group // 2 - x + 4) % 4) * 2 + (group % 2 + zl) % 2


def prep_kernel(
    q_ref, k_ref, v_ref, ids_ref, logit_ref, w_ref, kvsend_ref, back_ref, qnear_ref, cargo_ref
):
    x = lax.axis_index("x")
    zl = lax.axis_index("zl")
    spread = (iota((TOP, ROWS), 1) % TOP == iota((TOP, ROWS), 0)).astype(f32)
    own = iota((TOK, ROWS), 1) // TOP == iota((TOK, ROWS), 0)

    def as_row(table):
        wide = jnp.dot(table, spread, precision=lax.Precision.HIGHEST, preferred_element_type=f32)
        return jnp.sum(jnp.where(own, wide, 0.0), axis=0, keepdims=True)

    id_row = as_row(ids_ref[...].astype(f32))
    gate_exp = jnp.exp(logit_ref[...])
    gate_row = as_row(gate_exp / jnp.sum(gate_exp, axis=1, keepdims=True))
    id_int = id_row.astype(jnp.int32)
    id_col = jnp.broadcast_to(id_row, (ROWS, ROWS)).T
    earlier = (id_col == id_row) & (iota((ROWS, ROWS), 0) < iota((ROWS, ROWS), 1))
    rank = jnp.sum(earlier.astype(f32), axis=0, keepdims=True).astype(jnp.int32)
    group = id_int // PER
    within = (id_int % PER) * MOST + rank
    slot = away(group, x, zl) * SLOTS + within
    placed = (iota((GROUPS * SLOTS, ROWS), 0) == slot).astype(bf16)
    rows = jnp.dot(placed, q_ref[...], preferred_element_type=f32)
    tag_at = iota((8, ROWS), 0)
    tags = jnp.where(tag_at == 0, (iota((8, ROWS), 1) // TOP).astype(f32), 0.0)
    tags = jnp.where(tag_at == 1, gate_row, tags).astype(bf16)
    for g in range(GROUPS):
        here = (iota((ROWS, ROWS), 0) == slot - g * SLOTS).astype(bf16)
        info = lax.dot_general(tags, here, NT, preferred_element_type=f32)
        chunk = jnp.concatenate(
            [rows[g * SLOTS : g * SLOTS + PER * MOST], info], axis=0
        ).astype(bf16)
        if g % 2 == 0:
            qnear_ref[g // 2] = chunk
        else:
            cargo_ref[PER * HD + g // 2 * SLOTS : PER * HD + (g // 2 + 1) * SLOTS] = chunk
    cargo_ref[0 : PER * HD] = w_ref[...].reshape(PER * HD, HD)
    slot = group * SLOTS + within
    slot_col = jnp.broadcast_to(slot.astype(f32), (ROWS, ROWS)).T.astype(jnp.int32)
    lane = iota((ROWS, ROWS), 1)
    back_ref[:, :ROWS] = (lane == slot_col).astype(bf16)
    back_ref[:, ROWS:] = (lane + ROWS == slot_col).astype(bf16)
    keys = k_ref[...]
    values = v_ref[...]
    ids = jnp.broadcast_to(id_row, (8, ROWS)).astype(bf16)

    def fill(i, _):
        kvsend_ref[i, 0:SPAN] = keys
        kvsend_ref[i, SPAN : 2 * SPAN] = values
        kvsend_ref[i, 2 * SPAN : KVROWS] = ids
        return 0

    lax.fori_loop(0, CHIPS, fill, 0)


def attend_kernel(at_ref, kva_ref, kvb_ref, *refs):
    q_refs, (out_ref, s_ref) = refs[:4], refs[4:]
    n = GROUPS * SLOTS
    step = 4
    width = step * SPAN
    steps = CHIPS // step
    chunks = [
        q_refs[d // 2][d % 2 * SLOTS : (d % 2 + 1) * SLOTS] for d in range(GROUPS)
    ]
    queries = jnp.concatenate(chunks, axis=0)
    ctx = at_ref[0]
    core = at_ref[1]
    tags = jnp.concatenate(
        [chunk.astype(f32)[PER * MOST :] for chunk in chunks], axis=0
    )
    tags = jnp.concatenate([tags, tags], axis=0).T[0:SLOTS]
    token = jnp.concatenate([tags[:, g * 8 : g * 8 + 1] for g in range(GROUPS)], axis=0)
    gate = jnp.concatenate([tags[:, g * 8 + 1 : g * 8 + 2] for g in range(GROUPS)], axis=0)
    sources = [
        ((at_ref[2] - d // 2 + 4) % 4) * 2 + (at_ref[3] + d % 2) % 2 for d in range(GROUPS)
    ]
    source = jnp.concatenate([jnp.full((SLOTS, 1), d, jnp.int32) for d in sources], axis=0)
    pos = (source * (2 * CHIPS) + ctx) * TOK + token.astype(jnp.int32)
    scale = HD ** (-0.5) * math.log2(math.e)
    lane = iota((1, width), 1)

    def score(i, best, kv_ref, parity, base):
        keys = kv_ref[pl.ds(i * step, step), 0:SPAN, :].reshape(width, HD)
        scores = lax.dot_general(queries, keys, NT, preferred_element_type=f32) * scale
        key_pos = (2 * (i * step + lane // SPAN) + parity) * SPAN + lane % SPAN
        scores = jnp.where(key_pos <= pos, scores, NEG_FLOOR)
        s_ref[base + i] = scores
        return jnp.maximum(best, jnp.maximum(scores[:, :HD], scores[:, HD:]))

    def score_both(i, best):
        best = score(i, best, kva_ref, core, 0)
        return score(i, best, kvb_ref, 1 - core, steps)

    best = lax.fori_loop(0, steps, score_both, jnp.full((n, HD), NEG_FLOOR, f32))
    best = jnp.max(best, axis=1, keepdims=True)

    def weigh(i, carried, kv_ref, base):
        total, acc = carried
        exps = jnp.exp2(s_ref[base + i] - best)
        values = kv_ref[pl.ds(i * step, step), SPAN : 2 * SPAN, :].reshape(width, HD)
        acc = acc + jnp.dot(exps.astype(bf16), values, preferred_element_type=f32)
        return total + exps[:, :HD] + exps[:, HD:], acc

    def weigh_both(i, carried):
        return weigh(i, weigh(i, carried, kva_ref, 0), kvb_ref, steps)

    zero = jnp.zeros((n, HD), f32)
    total, acc = lax.fori_loop(0, steps, weigh_both, (zero, zero))
    total = jnp.sum(total, axis=1, keepdims=True)
    result = (gate * (acc / total)).astype(bf16)
    for d in range(GROUPS):
        out_ref[sources[d]] = result[d * SLOTS : (d + 1) * SLOTS]


def compact_kernel(back_ref, got_ref, out_ref):
    rows = jnp.dot(
        back_ref[...], got_ref[...].reshape(GROUPS * SLOTS, HD), preferred_element_type=f32
    ).astype(bf16)

    def fill(i, _):
        out_ref[i] = rows
        return 0

    lax.fori_loop(0, CHIPS, fill, 0)


def project_kernel(at_ref, rows_ref, kv_ref, *refs):
    mine_ref, other_ref, a_ref, w_ref, sems = refs[8:]
    copies = [pltpu.make_async_copy(refs[k], w_ref.at[k], sems.at[k]) for k in range(8)]
    for copy in copies:
        copy.start()
    x = at_ref[0]
    zl = at_ref[1]
    token = iota((1, ROWS), 1) // TOP
    target_at = iota((EXPERTS * TOK, ROWS), 0)

    def spread(i):
        ids = kv_ref[i, 2 * SPAN : KVROWS, :].astype(f32)[0:1].astype(jnp.int32)
        group = ids // PER
        piece = ((x - group // 2 + 4) % 4) * 2 + (group % 2 + zl) % 2
        target = (piece * PER + ids % PER) * TOK + token
        hot = (target_at == target).astype(bf16)
        got = jnp.dot(hot, rows_ref[i], preferred_element_type=f32)
        return got.reshape(EXPERTS, TOK, HD)

    def fill(i, _):
        both = jnp.concatenate([spread(2 * i), spread(2 * i + 1)], axis=1).astype(bf16)
        at = pl.ds(pl.multiple_of(i * 2 * TOK, 2 * TOK), 2 * TOK)
        for e in range(EXPERTS):
            a_ref[e // PER, at, (e % PER) * HD : (e % PER + 1) * HD] = both[e]
        return 0

    lax.fori_loop(0, CHIPS // 2, fill, 0)

    for copy in copies:
        copy.wait()
    total = jnp.zeros((CHIPS * TOK, 2 * HD), f32)
    for piece in range(GROUPS):
        part = slice(piece % 2 * PER, (piece % 2 + 1) * PER)
        near = w_ref[piece // 2, part].reshape(PER * HD, HD)
        far = w_ref[4 + piece // 2, part].reshape(PER * HD, HD)
        weight = jnp.concatenate([near, far], axis=1)
        total = total + jnp.dot(a_ref[piece], weight, preferred_element_type=f32)
    mine_ref[...] = total[:, :HD].astype(bf16)
    other_ref[...] = total[:, HD:].astype(bf16)


SMEM = pl.BlockSpec(memory_space=pltpu.SMEM)
VMEM = pl.BlockSpec(memory_space=pltpu.VMEM)
HBM = pl.BlockSpec(memory_space=pltpu.HBM)


def shifted(x, axis, count, by):
    return lax.ppermute(x, axis, [(i, (i + by) % count) for i in range(count)])


def run(queries, key_heads, value_heads, expert_ids, gate_logits, out_weight):
    zh, y, core = lax.axis_index("zh"), lax.axis_index("y"), lax.axis_index("core")
    x, zl = lax.axis_index("x"), lax.axis_index("zl")
    ctx = (zh * 8 + y) * 2 + core
    at = jnp.stack([ctx, core, x, zl]).astype(jnp.int32)
    at_exp = jnp.stack([x, zl, core]).astype(jnp.int32)
    shape = jax.ShapeDtypeStruct
    kvsend, back, qnear, cargo = pl.pallas_call(
        prep_kernel,
        in_specs=[VMEM] * 6,
        out_specs=[VMEM] * 4,
        out_shape=[
            shape((CHIPS, KVROWS, HD), bf16),
            shape((ROWS, GROUPS * SLOTS), bf16),
            shape((4, SLOTS, HD), bf16),
            shape((PER * HD + 4 * SLOTS, HD), bf16),
        ],
        name="prep",
    )(
        queries.reshape(ROWS, HD),
        key_heads.reshape(SPAN, HD),
        value_heads.reshape(SPAN, HD),
        expert_ids,
        gate_logits,
        out_weight,
    )
    kva = lax.all_to_all(kvsend, ("zh", "y"), 0, 0, tiled=True)
    got = shifted(cargo, "zl", 2, 1)
    crossed = got[PER * HD :].reshape(4, SLOTS, HD)
    qpair = jnp.concatenate([qnear, crossed], axis=1)
    qgot = [qpair[k] for k in range(4)]
    for k in range(1, 4):
        qgot[k] = shifted(qgot[k], "x", 4, k)
    pair = jnp.concatenate([out_weight, got[: PER * HD].reshape(PER, HD, HD)], axis=0)
    pieces = [pair]
    for k in range(1, 4):
        pieces.append(shifted(pair, "x", 4, k))
    far = []
    for k in range(4):
        far.append(shifted(pieces[k], "core", 2, 1))
    kvb = shifted(kva, "core", 2, 1)
    attended = pl.pallas_call(
        attend_kernel,
        in_specs=[SMEM] + [VMEM] * 6,
        out_specs=VMEM,
        out_shape=shape((GROUPS, SLOTS, HD), bf16),
        scratch_shapes=[pltpu.VMEM((16, GROUPS * SLOTS, 4 * SPAN), f32)],
        compiler_params=pltpu.CompilerParams(vmem_limit_bytes=14 << 20),
        name="attend",
    )(at, kva, kvb, *qgot)
    home = lax.all_to_all(attended, ("x", "zl"), 0, 0, tiled=True)
    rows = pl.pallas_call(
        compact_kernel,
        in_specs=[VMEM, VMEM],
        out_specs=VMEM,
        out_shape=shape((CHIPS, ROWS, HD), bf16),
        compiler_params=pltpu.CompilerParams(vmem_limit_bytes=8 << 20),
        name="compact",
    )(back, home)
    rows = lax.all_to_all(rows, ("zh", "y"), 0, 0, tiled=True)
    mine, other = pl.pallas_call(
        project_kernel,
        in_specs=[SMEM] + [VMEM] * 2 + [HBM] * 8,
        out_specs=[VMEM, VMEM],
        out_shape=[shape((CHIPS * TOK, HD), bf16)] * 2,
        scratch_shapes=[
            pltpu.VMEM((GROUPS, CHIPS * TOK, PER * HD), bf16),
            pltpu.VMEM((8, 2 * PER, HD, HD), bf16),
            pltpu.SemaphoreType.DMA((8,)),
        ],
        compiler_params=pltpu.CompilerParams(vmem_limit_bytes=58 << 20),
        name="project",
    )(at_exp, rows, kva, *pieces, *far)
    got = shifted(other, "core", 2, 1)
    own = lax.broadcasted_iota(jnp.int32, (CHIPS, 2, TOK, HD), 1) == core
    mine = mine.reshape(CHIPS, 1, TOK, HD)
    got = got.reshape(CHIPS, 1, TOK, HD)
    return jnp.where(own, mine, got).reshape(2 * CHIPS * TOK, HD)


def solution(mesh):
    fine = Mesh(mesh.devices.reshape(4, 8, 2, 4, 2), ("zh", "y", "core", "x", "zl"))
    ctx, exp = ("zh", "y", "core"), ("x", "zl")
    in_specs = (
        P(exp + ctx, None, None),
        P(ctx, exp, None),
        P(ctx, exp, None),
        P(exp + ctx, None),
        P(exp + ctx, None),
        P(exp, None, ctx),
    )
    return jax.shard_map(run, mesh=fine, in_specs=in_specs, out_specs=P(exp, ctx), check_vma=False)
```

```python
import math

import jax
import jax.numpy as jnp
from jax import lax
from jax.experimental import pallas as pl
from jax.experimental.pallas import tpu as pltpu
from jax.sharding import Mesh, PartitionSpec as P


EXPERTS = 64
HD = 128
TOP = 16
MOST = 3
TOK = 8
ROWS = TOK * TOP
GROUPS = 8
PER = EXPERTS // GROUPS
SLOTS = 32
SPAN = 64
CHIPS = 32
KVROWS = 2 * SPAN + 8
NEG_FLOOR = -1e30


f32 = jnp.float32
bf16 = jnp.bfloat16
NT = (((1,), (1,)), ((), ()))


def iota(shape, dim):
    return lax.broadcasted_iota(jnp.int32, shape, dim)


def away(group, x, zl):
    return ((group // 2 - x + 4) % 4) * 2 + (group % 2 + zl) % 2


def prep_kernel(
    q_ref, k_ref, v_ref, ids_ref, logit_ref, w_ref, kvsend_ref, back_ref, qnear_ref, cargo_ref
):
    x = lax.axis_index("x")
    zl = lax.axis_index("zl")
    spread = (iota((TOP, ROWS), 1) % TOP == iota((TOP, ROWS), 0)).astype(f32)
    own = iota((TOK, ROWS), 1) // TOP == iota((TOK, ROWS), 0)

    def as_row(table):
        wide = jnp.dot(table, spread, precision=lax.Precision.HIGHEST, preferred_element_type=f32)
        return jnp.sum(jnp.where(own, wide, 0.0), axis=0, keepdims=True)

    id_row = as_row(ids_ref[...].astype(f32))
    gate_exp = jnp.exp(logit_ref[...])
    gate_row = as_row(gate_exp / jnp.sum(gate_exp, axis=1, keepdims=True))
    id_int = id_row.astype(jnp.int32)
    id_col = jnp.broadcast_to(id_row, (ROWS, ROWS)).T
    earlier = (id_col == id_row) & (iota((ROWS, ROWS), 0) < iota((ROWS, ROWS), 1))
    rank = jnp.sum(earlier.astype(f32), axis=0, keepdims=True).astype(jnp.int32)
    group = id_int // PER
    within = (id_int % PER) * MOST + rank
    slot = away(group, x, zl) * SLOTS + within
    placed = (iota((GROUPS * SLOTS, ROWS), 0) == slot).astype(bf16)
    rows = jnp.dot(placed, q_ref[...], preferred_element_type=f32)
    tag_at = iota((8, ROWS), 0)
    tags = jnp.where(tag_at == 0, (iota((8, ROWS), 1) // TOP).astype(f32), 0.0)
    tags = jnp.where(tag_at == 1, gate_row, tags).astype(bf16)
    for g in range(GROUPS):
        here = (iota((ROWS, ROWS), 0) == slot - g * SLOTS).astype(bf16)
        info = lax.dot_general(tags, here, NT, preferred_element_type=f32)
        chunk = jnp.concatenate(
            [rows[g * SLOTS : g * SLOTS + PER * MOST], info], axis=0
        ).astype(bf16)
        if g % 2 == 0:
            qnear_ref[g // 2] = chunk
        else:
            cargo_ref[PER * HD + g // 2 * SLOTS : PER * HD + (g // 2 + 1) * SLOTS] = chunk
    cargo_ref[0 : PER * HD] = w_ref[...].reshape(PER * HD, HD)
    slot = group * SLOTS + within
    slot_col = jnp.broadcast_to(slot.astype(f32), (ROWS, ROWS)).T.astype(jnp.int32)
    lane = iota((ROWS, ROWS), 1)
    back_ref[:, :ROWS] = (lane == slot_col).astype(bf16)
    back_ref[:, ROWS:] = (lane + ROWS == slot_col).astype(bf16)
    keys = k_ref[...]
    values = v_ref[...]
    ids = jnp.broadcast_to(id_row, (8, ROWS)).astype(bf16)

    def fill(i, _):
        kvsend_ref[i, 0:SPAN] = keys
        kvsend_ref[i, SPAN : 2 * SPAN] = values
        kvsend_ref[i, 2 * SPAN : KVROWS] = ids
        return 0

    lax.fori_loop(0, CHIPS, fill, 0)


def attend_kernel(at_ref, kva_ref, kvb_ref, *refs):
    q_refs, (out_ref, s_ref) = refs[:4], refs[4:]
    n = GROUPS * SLOTS
    step = 4
    width = step * SPAN
    steps = CHIPS // step
    chunks = [
        q_refs[d // 2][d % 2 * SLOTS : (d % 2 + 1) * SLOTS] for d in range(GROUPS)
    ]
    queries = jnp.concatenate(chunks, axis=0)
    ctx = at_ref[0]
    core = at_ref[1]
    tags = jnp.concatenate(
        [chunk.astype(f32)[PER * MOST :] for chunk in chunks], axis=0
    )
    tags = jnp.concatenate([tags, tags], axis=0).T[0:SLOTS]
    token = jnp.concatenate([tags[:, g * 8 : g * 8 + 1] for g in range(GROUPS)], axis=0)
    gate = jnp.concatenate([tags[:, g * 8 + 1 : g * 8 + 2] for g in range(GROUPS)], axis=0)
    sources = [
        ((at_ref[2] - d // 2 + 4) % 4) * 2 + (at_ref[3] + d % 2) % 2 for d in range(GROUPS)
    ]
    source = jnp.concatenate([jnp.full((SLOTS, 1), d, jnp.int32) for d in sources], axis=0)
    pos = (source * (2 * CHIPS) + ctx) * TOK + token.astype(jnp.int32)
    scale = HD ** (-0.5) * math.log2(math.e)
    lane = iota((1, width), 1)

    def score(i, best, kv_ref, parity, base):
        keys = kv_ref[pl.ds(i * step, step), 0:SPAN, :].reshape(width, HD)
        scores = lax.dot_general(queries, keys, NT, preferred_element_type=f32) * scale
        key_pos = (2 * (i * step + lane // SPAN) + parity) * SPAN + lane % SPAN
        scores = jnp.where(key_pos <= pos, scores, NEG_FLOOR)
        s_ref[base + i] = scores
        return jnp.maximum(best, jnp.maximum(scores[:, :HD], scores[:, HD:]))

    def score_both(i, best):
        best = score(i, best, kva_ref, core, 0)
        return score(i, best, kvb_ref, 1 - core, steps)

    best = lax.fori_loop(
        0, steps, score_both, jnp.full((n, HD), NEG_FLOOR, f32), unroll=4
    )
    best = jnp.max(best, axis=1, keepdims=True)

    def weigh(i, carried, kv_ref, base):
        total, acc = carried
        exps = jnp.exp2(s_ref[base + i] - best)
        values = kv_ref[pl.ds(i * step, step), SPAN : 2 * SPAN, :].reshape(width, HD)
        acc = acc + jnp.dot(exps.astype(bf16), values, preferred_element_type=f32)
        return total + exps[:, :HD] + exps[:, HD:], acc

    def weigh_both(i, carried):
        return weigh(i, weigh(i, carried, kva_ref, 0), kvb_ref, steps)

    zero = jnp.zeros((n, HD), f32)
    total, acc = lax.fori_loop(0, steps, weigh_both, (zero, zero), unroll=4)
    total = jnp.sum(total, axis=1, keepdims=True)
    result = (gate * (acc / total)).astype(bf16)
    for d in range(GROUPS):
        out_ref[sources[d]] = result[d * SLOTS : (d + 1) * SLOTS]


def compact_kernel(back_ref, got_ref, out_ref):
    rows = jnp.dot(
        back_ref[...], got_ref[...].reshape(GROUPS * SLOTS, HD), preferred_element_type=f32
    ).astype(bf16)

    def fill(i, _):
        out_ref[i] = rows
        return 0

    lax.fori_loop(0, CHIPS, fill, 0)


def project_kernel(at_ref, rows_ref, kv_ref, *refs):
    mine_ref, other_ref, a_ref, w_ref, sems = refs[2:]
    copies = [pltpu.make_async_copy(refs[k], w_ref.at[k], sems.at[k]) for k in range(2)]
    for copy in copies:
        copy.start()
    x = at_ref[0]
    zl = at_ref[1]
    token = iota((1, ROWS), 1) // TOP
    target_at = iota((EXPERTS * TOK, ROWS), 0)

    def spread(i):
        ids = kv_ref[i, 2 * SPAN : KVROWS, :].astype(f32)[0:1].astype(jnp.int32)
        group = ids // PER
        piece = ((x - group // 2 + 4) % 4) * 2 + (group % 2 + zl) % 2
        target = (piece * PER + ids % PER) * TOK + token
        hot = (target_at == target).astype(bf16)
        got = jnp.dot(hot, rows_ref[i], preferred_element_type=f32)
        return got.reshape(EXPERTS, TOK, HD)

    def fill(i, _):
        both = jnp.concatenate([spread(2 * i), spread(2 * i + 1)], axis=1).astype(bf16)
        at = pl.ds(pl.multiple_of(i * 2 * TOK, 2 * TOK), 2 * TOK)
        for e in range(EXPERTS):
            a_ref[e // PER, at, (e % PER) * HD : (e % PER + 1) * HD] = both[e]
        return 0

    lax.fori_loop(0, CHIPS // 2, fill, 0, unroll=4)

    for copy in copies:
        copy.wait()
    total = jnp.zeros((CHIPS * TOK, 2 * HD), f32)
    for piece in range(GROUPS):
        part = slice(piece * PER, (piece + 1) * PER)
        near = w_ref[0, part].reshape(PER * HD, HD)
        far = w_ref[1, part].reshape(PER * HD, HD)
        weight = jnp.concatenate([near, far], axis=1)
        total = total + jnp.dot(a_ref[piece], weight, preferred_element_type=f32)
    mine_ref[...] = total[:, :HD].astype(bf16)
    other_ref[...] = total[:, HD:].astype(bf16)


SMEM = pl.BlockSpec(memory_space=pltpu.SMEM)
VMEM = pl.BlockSpec(memory_space=pltpu.VMEM)
HBM = pl.BlockSpec(memory_space=pltpu.HBM)


def shifted(x, axis, count, by):
    return lax.ppermute(x, axis, [(i, (i + by) % count) for i in range(count)])


def run(queries, key_heads, value_heads, expert_ids, gate_logits, out_weight):
    zh, y, core = lax.axis_index("zh"), lax.axis_index("y"), lax.axis_index("core")
    x, zl = lax.axis_index("x"), lax.axis_index("zl")
    ctx = (zh * 8 + y) * 2 + core
    at = jnp.stack([ctx, core, x, zl]).astype(jnp.int32)
    at_exp = jnp.stack([x, zl, core]).astype(jnp.int32)
    shape = jax.ShapeDtypeStruct
    kvsend, back, qnear, cargo = pl.pallas_call(
        prep_kernel,
        in_specs=[VMEM] * 6,
        out_specs=[VMEM] * 4,
        out_shape=[
            shape((CHIPS, KVROWS, HD), bf16),
            shape((ROWS, GROUPS * SLOTS), bf16),
            shape((4, SLOTS, HD), bf16),
            shape((PER * HD + 4 * SLOTS, HD), bf16),
        ],
        name="prep",
    )(
        queries.reshape(ROWS, HD),
        key_heads.reshape(SPAN, HD),
        value_heads.reshape(SPAN, HD),
        expert_ids,
        gate_logits,
        out_weight,
    )
    kva = lax.all_to_all(kvsend, ("zh", "y"), 0, 0, tiled=True)
    got = shifted(cargo, "zl", 2, 1)
    crossed = got[PER * HD :].reshape(4, SLOTS, HD)
    qpair = jnp.concatenate([qnear, crossed], axis=1)
    qgot = [qpair[k] for k in range(4)]
    for k in range(1, 4):
        qgot[k] = shifted(qgot[k], "x", 4, k)
    pair = jnp.concatenate([out_weight, got[: PER * HD].reshape(PER, HD, HD)], axis=0)
    pieces = [pair]
    for k in range(1, 4):
        pieces.append(shifted(pair, "x", 4, k))
    near = jnp.concatenate(pieces, axis=0)
    far = shifted(near, "core", 2, 1)
    kvb = shifted(kva, "core", 2, 1)
    attended = pl.pallas_call(
        attend_kernel,
        in_specs=[SMEM] + [VMEM] * 6,
        out_specs=VMEM,
        out_shape=shape((GROUPS, SLOTS, HD), bf16),
        scratch_shapes=[pltpu.VMEM((16, GROUPS * SLOTS, 4 * SPAN), f32)],
        compiler_params=pltpu.CompilerParams(vmem_limit_bytes=14 << 20),
        name="attend",
    )(at, kva, kvb, *qgot)
    home = lax.all_to_all(attended, ("x", "zl"), 0, 0, tiled=True)
    rows = pl.pallas_call(
        compact_kernel,
        in_specs=[VMEM, VMEM],
        out_specs=VMEM,
        out_shape=shape((CHIPS, ROWS, HD), bf16),
        compiler_params=pltpu.CompilerParams(vmem_limit_bytes=8 << 20),
        name="compact",
    )(back, home)
    rows = lax.all_to_all(rows, ("zh", "y"), 0, 0, tiled=True)
    mine, other = pl.pallas_call(
        project_kernel,
        in_specs=[SMEM] + [VMEM] * 2 + [HBM] * 2,
        out_specs=[VMEM, VMEM],
        out_shape=[shape((CHIPS * TOK, HD), bf16)] * 2,
        scratch_shapes=[
            pltpu.VMEM((GROUPS, CHIPS * TOK, PER * HD), bf16),
            pltpu.VMEM((2, EXPERTS, HD, HD), bf16),
            pltpu.SemaphoreType.DMA((2,)),
        ],
        compiler_params=pltpu.CompilerParams(vmem_limit_bytes=50 << 20),
        name="project",
    )(at_exp, rows, kva, near, far)
    got = shifted(other, "core", 2, 1)
    own = lax.broadcasted_iota(jnp.int32, (CHIPS, 2, TOK, HD), 1) == core
    mine = mine.reshape(CHIPS, 1, TOK, HD)
    got = got.reshape(CHIPS, 1, TOK, HD)
    return jnp.where(own, mine, got).reshape(2 * CHIPS * TOK, HD)


def solution(mesh):
    fine = Mesh(mesh.devices.reshape(4, 8, 2, 4, 2), ("zh", "y", "core", "x", "zl"))
    ctx, exp = ("zh", "y", "core"), ("x", "zl")
    in_specs = (
        P(exp + ctx, None, None),
        P(ctx, exp, None),
        P(ctx, exp, None),
        P(exp + ctx, None),
        P(exp + ctx, None),
        P(exp, None, ctx),
    )
    return jax.shard_map(run, mesh=fine, in_specs=in_specs, out_specs=P(exp, ctx), check_vma=False)
```

```python
import math

import jax
import jax.numpy as jnp
from jax import lax
from jax.experimental import pallas as pl
from jax.experimental.pallas import tpu as pltpu
from jax.sharding import Mesh, PartitionSpec as P


EXPERTS = 64
HD = 128
TOP = 16
MOST = 3
TOK = 8
ROWS = TOK * TOP
GROUPS = 8
PER = EXPERTS // GROUPS
SLOTS = 32
SPAN = 64
CHIPS = 32
KVROWS = 2 * SPAN + 8
NEG_FLOOR = -1e30


f32 = jnp.float32
bf16 = jnp.bfloat16
NT = (((1,), (1,)), ((), ()))


def iota(shape, dim):
    return lax.broadcasted_iota(jnp.int32, shape, dim)


def away(group, x, zl):
    return ((group // 2 - x + 4) % 4) * 2 + (group % 2 + zl) % 2


def prep_kernel(
    q_ref, k_ref, v_ref, ids_ref, logit_ref, w_ref, kvsend_ref, back_ref, qnear_ref, cargo_ref
):
    x = lax.axis_index("x")
    zl = lax.axis_index("zl")
    spread = (iota((TOP, ROWS), 1) % TOP == iota((TOP, ROWS), 0)).astype(bf16)
    own = iota((TOK, ROWS), 1) // TOP == iota((TOK, ROWS), 0)

    def as_row(table):
        wide = jnp.dot(table.astype(bf16), spread, preferred_element_type=f32)
        return jnp.sum(jnp.where(own, wide, 0.0), axis=0, keepdims=True)

    id_row = as_row(ids_ref[...].astype(f32))
    gate_exp = jnp.exp(logit_ref[...])
    gate_row = as_row(gate_exp / jnp.sum(gate_exp, axis=1, keepdims=True))
    id_int = id_row.astype(jnp.int32)
    id_col = jnp.broadcast_to(id_row, (ROWS, ROWS)).T
    earlier = (id_col == id_row) & (iota((ROWS, ROWS), 0) < iota((ROWS, ROWS), 1))
    rank = jnp.sum(earlier.astype(f32), axis=0, keepdims=True).astype(jnp.int32)
    group = id_int // PER
    within = (id_int % PER) * MOST + rank
    slot = away(group, x, zl) * SLOTS + within
    placed = (iota((GROUPS * SLOTS, ROWS), 0) == slot).astype(bf16)
    rows = jnp.dot(placed, q_ref[...], preferred_element_type=f32)
    tag_at = iota((8, ROWS), 0)
    tags = jnp.where(tag_at == 0, (iota((8, ROWS), 1) // TOP).astype(f32), 0.0)
    tags = jnp.where(tag_at == 1, gate_row, tags).astype(bf16)
    for g in range(GROUPS):
        here = (iota((ROWS, ROWS), 0) == slot - g * SLOTS).astype(bf16)
        info = lax.dot_general(tags, here, NT, preferred_element_type=f32)
        chunk = jnp.concatenate(
            [rows[g * SLOTS : g * SLOTS + PER * MOST], info], axis=0
        ).astype(bf16)
        if g % 2 == 0:
            qnear_ref[g // 2] = chunk
        else:
            cargo_ref[PER * HD + g // 2 * SLOTS : PER * HD + (g // 2 + 1) * SLOTS] = chunk
    cargo_ref[0 : PER * HD] = w_ref[...].reshape(PER * HD, HD)
    slot = group * SLOTS + within
    slot_col = jnp.broadcast_to(slot.astype(f32), (ROWS, ROWS)).T.astype(jnp.int32)
    lane = iota((ROWS, ROWS), 1)
    back_ref[:, :ROWS] = (lane == slot_col).astype(bf16)
    back_ref[:, ROWS:] = (lane + ROWS == slot_col).astype(bf16)
    keys = k_ref[...]
    values = v_ref[...]
    ids = jnp.broadcast_to(id_row, (8, ROWS)).astype(bf16)

    def fill(i, _):
        kvsend_ref[i, 0:SPAN] = keys
        kvsend_ref[i, SPAN : 2 * SPAN] = values
        kvsend_ref[i, 2 * SPAN : KVROWS] = ids
        return 0

    lax.fori_loop(0, CHIPS, fill, 0)


def attend_half(at_ref, kv_ref, q_refs, s_ref, parity, best):
    n = GROUPS * SLOTS
    step = 4
    width = step * SPAN
    steps = CHIPS // step
    chunks = [
        q_refs[d // 2][d % 2 * SLOTS : (d % 2 + 1) * SLOTS] for d in range(GROUPS)
    ]
    queries = jnp.concatenate(chunks, axis=0)
    ctx = at_ref[0]
    tags = jnp.concatenate([chunk.astype(f32)[PER * MOST :] for chunk in chunks], axis=0)
    tags = jnp.concatenate([tags, tags], axis=0).T[0:SLOTS]
    token = jnp.concatenate([tags[:, g * 8 : g * 8 + 1] for g in range(GROUPS)], axis=0)
    gate = jnp.concatenate([tags[:, g * 8 + 1 : g * 8 + 2] for g in range(GROUPS)], axis=0)
    sources = [
        ((at_ref[2] - d // 2 + 4) % 4) * 2 + (at_ref[3] + d % 2) % 2 for d in range(GROUPS)
    ]
    source = jnp.concatenate([jnp.full((SLOTS, 1), d, jnp.int32) for d in sources], axis=0)
    pos = (source * (2 * CHIPS) + ctx) * TOK + token.astype(jnp.int32)
    scale = HD ** (-0.5) * math.log2(math.e)
    lane = iota((1, width), 1)

    def score(i, top):
        keys = kv_ref[pl.ds(i * step, step), 0:SPAN, :].reshape(width, HD)
        scores = lax.dot_general(queries, keys, NT, preferred_element_type=f32) * scale
        key_pos = (2 * (i * step + lane // SPAN) + parity) * SPAN + lane % SPAN
        scores = jnp.where(key_pos <= pos, scores, NEG_FLOOR)
        s_ref[i] = scores
        return jnp.maximum(top, jnp.maximum(scores[:, :HD], scores[:, HD:]))

    best = lax.fori_loop(0, steps, score, best, unroll=8)
    best = jnp.max(best, axis=1, keepdims=True)

    def weigh(i, carried):
        total, acc = carried
        scores = s_ref[i]
        exps = jnp.where(scores > 0.5 * NEG_FLOOR, jnp.exp2(scores - best), 0.0)
        values = kv_ref[pl.ds(i * step, step), SPAN : 2 * SPAN, :].reshape(width, HD)
        acc = acc + jnp.dot(exps.astype(bf16), values, preferred_element_type=f32)
        return total + exps[:, :HD] + exps[:, HD:], acc

    zero = jnp.zeros((n, HD), f32)
    total, acc = lax.fori_loop(0, steps, weigh, (zero, zero), unroll=8)
    return best, total, acc, gate, sources


def attend_own_kernel(at_ref, kv_ref, *refs):
    q_refs, (best_ref, total_ref, acc_ref, s_ref) = refs[:4], refs[4:]
    best = jnp.full((GROUPS * SLOTS, HD), NEG_FLOOR, f32)
    best, total, acc, _, _ = attend_half(at_ref, kv_ref, q_refs, s_ref, at_ref[1], best)
    best_ref[...] = jnp.broadcast_to(best, acc.shape)
    total_ref[...] = total
    acc_ref[...] = acc


def attend_kernel(at_ref, kv_ref, *refs):
    q_refs, (best_ref, total_ref, acc_ref, out_ref, s_ref) = refs[:4], refs[4:]
    before = best_ref[...]
    best, total, acc, gate, sources = attend_half(
        at_ref, kv_ref, q_refs, s_ref, 1 - at_ref[1], before
    )
    fade = jnp.exp2(before - best)
    total = jnp.sum(total + total_ref[...] * fade, axis=1, keepdims=True)
    acc = acc + acc_ref[...] * fade
    result = (gate * (acc / total)).astype(bf16)
    for d in range(GROUPS):
        out_ref[sources[d]] = result[d * SLOTS : (d + 1) * SLOTS]


def compact_kernel(back_ref, got_ref, out_ref):
    rows = jnp.dot(
        back_ref[...], got_ref[...].reshape(GROUPS * SLOTS, HD), preferred_element_type=f32
    ).astype(bf16)

    def fill(i, _):
        out_ref[i] = rows
        return 0

    lax.fori_loop(0, CHIPS, fill, 0)


def join_kernel(*refs):
    out_ref, sems = refs[4:]
    copies = [
        pltpu.make_async_copy(refs[k], out_ref.at[pl.ds(k * 2 * PER, 2 * PER)], sems.at[k])
        for k in range(4)
    ]
    for copy in copies:
        copy.start()
    for copy in copies:
        copy.wait()


def project_kernel(at_ref, rows_ref, kv_ref, *refs):
    mine_ref, other_ref, a_ref, w_ref, sems = refs[2:]
    copies = [pltpu.make_async_copy(refs[k], w_ref.at[k], sems.at[k]) for k in range(2)]
    for copy in copies:
        copy.start()
    x = at_ref[0]
    zl = at_ref[1]
    token = iota((1, ROWS), 1) // TOP
    target_at = iota((EXPERTS * TOK, ROWS), 0)

    def spread(i):
        ids = kv_ref[i, 2 * SPAN : KVROWS, :].astype(f32)[0:1].astype(jnp.int32)
        group = ids // PER
        piece = ((x - group // 2 + 4) % 4) * 2 + (group % 2 + zl) % 2
        target = (piece * PER + ids % PER) * TOK + token
        hot = (target_at == target).astype(bf16)
        got = jnp.dot(hot, rows_ref[i], preferred_element_type=f32)
        return got.reshape(EXPERTS, TOK, HD)

    def fill(i, _):
        both = jnp.concatenate([spread(2 * i), spread(2 * i + 1)], axis=1).astype(bf16)
        at = pl.ds(pl.multiple_of(i * 2 * TOK, 2 * TOK), 2 * TOK)
        for e in range(EXPERTS):
            a_ref[e // PER, at, (e % PER) * HD : (e % PER + 1) * HD] = both[e]
        return 0

    lax.fori_loop(0, CHIPS // 2, fill, 0, unroll=4)

    for copy in copies:
        copy.wait()
    total = jnp.zeros((CHIPS * TOK, 2 * HD), f32)
    for piece in range(GROUPS):
        part = slice(piece * PER, (piece + 1) * PER)
        near = w_ref[0, part].reshape(PER * HD, HD)
        far = w_ref[1, part].reshape(PER * HD, HD)
        weight = jnp.concatenate([near, far], axis=1)
        total = total + jnp.dot(a_ref[piece], weight, preferred_element_type=f32)
    mine_ref[...] = total[:, :HD].astype(bf16)
    other_ref[...] = total[:, HD:].astype(bf16)


SMEM = pl.BlockSpec(memory_space=pltpu.SMEM)
VMEM = pl.BlockSpec(memory_space=pltpu.VMEM)
ANY = pl.BlockSpec(memory_space=pl.ANY)
HBM = pl.BlockSpec(memory_space=pltpu.HBM)


def shifted(x, axis, count, by):
    return lax.ppermute(x, axis, [(i, (i + by) % count) for i in range(count)])


def run(queries, key_heads, value_heads, expert_ids, gate_logits, out_weight):
    zh, y, core = lax.axis_index("zh"), lax.axis_index("y"), lax.axis_index("core")
    x, zl = lax.axis_index("x"), lax.axis_index("zl")
    ctx = (zh * 8 + y) * 2 + core
    at = jnp.stack([ctx, core, x, zl]).astype(jnp.int32)
    at_exp = jnp.stack([x, zl, core]).astype(jnp.int32)
    shape = jax.ShapeDtypeStruct
    kvsend, back, qnear, cargo = pl.pallas_call(
        prep_kernel,
        in_specs=[VMEM] * 6,
        out_specs=[VMEM] * 4,
        out_shape=[
            shape((CHIPS, KVROWS, HD), bf16),
            shape((ROWS, GROUPS * SLOTS), bf16),
            shape((4, SLOTS, HD), bf16),
            shape((PER * HD + 4 * SLOTS, HD), bf16),
        ],
        name="prep",
    )(
        queries.reshape(ROWS, HD),
        key_heads.reshape(SPAN, HD),
        value_heads.reshape(SPAN, HD),
        expert_ids,
        gate_logits,
        out_weight,
    )
    kva = lax.all_to_all(kvsend, ("zh", "y"), 0, 0, tiled=True)
    got = shifted(cargo, "zl", 2, 1)
    crossed = got[PER * HD :].reshape(4, SLOTS, HD)
    qpair = jnp.concatenate([qnear, crossed], axis=1)
    qgot = [qpair[k] for k in range(4)]
    for k in range(1, 4):
        qgot[k] = shifted(qgot[k], "x", 4, k)
    pair = jnp.concatenate([out_weight, got[: PER * HD].reshape(PER, HD, HD)], axis=0)
    pieces = [pair]
    for k in range(1, 4):
        pieces.append(shifted(pair, "x", 4, k))
    near = pl.pallas_call(
        join_kernel,
        in_specs=[ANY] * 4,
        out_specs=ANY,
        out_shape=shape((EXPERTS, HD, HD), bf16),
        scratch_shapes=[pltpu.SemaphoreType.DMA((4,))],
        compiler_params=pltpu.CompilerParams(vmem_limit_bytes=4 << 20),
        name="join",
    )(*pieces)
    far = shifted(near, "core", 2, 1)
    kvb = shifted(kva, "core", 2, 1)
    state = shape((GROUPS * SLOTS, HD), f32)
    scratch = [pltpu.VMEM((8, GROUPS * SLOTS, 4 * SPAN), f32)]
    running = pl.pallas_call(
        attend_own_kernel,
        in_specs=[SMEM] + [VMEM] * 5,
        out_specs=[VMEM] * 3,
        out_shape=[state] * 3,
        scratch_shapes=scratch,
        compiler_params=pltpu.CompilerParams(vmem_limit_bytes=14 << 20),
        name="attend_own",
    )(at, kva, *qgot)
    attended = pl.pallas_call(
        attend_kernel,
        in_specs=[SMEM] + [VMEM] * 8,
        out_specs=VMEM,
        out_shape=shape((GROUPS, SLOTS, HD), bf16),
        scratch_shapes=scratch,
        compiler_params=pltpu.CompilerParams(vmem_limit_bytes=14 << 20),
        name="attend",
    )(at, kvb, *qgot, *running)
    home = lax.all_to_all(attended, ("x", "zl"), 0, 0, tiled=True)
    rows = pl.pallas_call(
        compact_kernel,
        in_specs=[VMEM, VMEM],
        out_specs=VMEM,
        out_shape=shape((CHIPS, ROWS, HD), bf16),
        compiler_params=pltpu.CompilerParams(vmem_limit_bytes=8 << 20),
        name="compact",
    )(back, home)
    rows = lax.all_to_all(rows, ("zh", "y"), 0, 0, tiled=True)
    mine, other = pl.pallas_call(
        project_kernel,
        in_specs=[SMEM] + [VMEM] * 2 + [HBM] * 2,
        out_specs=[VMEM, VMEM],
        out_shape=[shape((CHIPS * TOK, HD), bf16)] * 2,
        scratch_shapes=[
            pltpu.VMEM((GROUPS, CHIPS * TOK, PER * HD), bf16),
            pltpu.VMEM((2, EXPERTS, HD, HD), bf16),
            pltpu.SemaphoreType.DMA((2,)),
        ],
        compiler_params=pltpu.CompilerParams(vmem_limit_bytes=48 << 20),
        name="project",
    )(at_exp, rows, kva, near, far)
    got = shifted(other, "core", 2, 1)
    own = lax.broadcasted_iota(jnp.int32, (CHIPS, 2, TOK, HD), 1) == core
    mine = mine.reshape(CHIPS, 1, TOK, HD)
    got = got.reshape(CHIPS, 1, TOK, HD)
    return jnp.where(own, mine, got).reshape(2 * CHIPS * TOK, HD)


def solution(mesh):
    fine = Mesh(mesh.devices.reshape(4, 8, 2, 4, 2), ("zh", "y", "core", "x", "zl"))
    ctx, exp = ("zh", "y", "core"), ("x", "zl")
    in_specs = (
        P(exp + ctx, None, None),
        P(ctx, exp, None),
        P(ctx, exp, None),
        P(exp + ctx, None),
        P(exp + ctx, None),
        P(exp, None, ctx),
    )
    return jax.shard_map(run, mesh=fine, in_specs=in_specs, out_specs=P(exp, ctx), check_vma=False)
```

```python
import math

import jax
import jax.numpy as jnp
from jax import lax
from jax.experimental import pallas as pl
from jax.experimental.pallas import tpu as pltpu
from jax.sharding import Mesh, PartitionSpec as P


EXPERTS = 64
HD = 128
TOP = 16
MOST = 3
TOK = 8
ROWS = TOK * TOP
GROUPS = 8
PER = EXPERTS // GROUPS
SLOTS = 32
SPAN = 64
CHIPS = 32
KVROWS = 2 * SPAN + 8
NEG_FLOOR = -1e30


f32 = jnp.float32
bf16 = jnp.bfloat16
NT = (((1,), (1,)), ((), ()))


def iota(shape, dim):
    return lax.broadcasted_iota(jnp.int32, shape, dim)


def away(group, x, zl):
    return ((group // 2 - x + 4) % 4) * 2 + (group % 2 + zl) % 2


def spread_tables():
    wide = (iota((TOP, ROWS), 1) % TOP == iota((TOP, ROWS), 0)).astype(bf16)
    own = iota((TOK, ROWS), 1) // TOP == iota((TOK, ROWS), 0)

    def as_row(table):
        every = jnp.dot(table.astype(bf16), wide, preferred_element_type=f32)
        return jnp.sum(jnp.where(own, every, 0.0), axis=0, keepdims=True)

    return as_row


def prep_kv_kernel(k_ref, v_ref, ids_ref, kvsend_ref, chunk_ref, sems):
    id_row = spread_tables()(ids_ref[...].astype(f32))
    chunk_ref[0:SPAN] = k_ref[...]
    chunk_ref[SPAN : 2 * SPAN] = v_ref[...]
    chunk_ref[2 * SPAN : KVROWS] = jnp.broadcast_to(id_row, (8, ROWS)).astype(bf16)
    copies = [
        pltpu.make_async_copy(chunk_ref, kvsend_ref.at[i], sems.at[i]) for i in range(CHIPS)
    ]
    for copy in copies:
        copy.start()
    for copy in copies:
        copy.wait()


def prep_q_kernel(q_ref, ids_ref, logit_ref, back_ref, qsend_ref):
    x = lax.axis_index("x")
    zl = lax.axis_index("zl")
    as_row = spread_tables()
    id_row = as_row(ids_ref[...].astype(f32))
    gate_exp = jnp.exp(logit_ref[...])
    gate_row = as_row(gate_exp / jnp.sum(gate_exp, axis=1, keepdims=True))
    id_int = id_row.astype(jnp.int32)
    id_col = jnp.broadcast_to(id_row, (ROWS, ROWS)).T
    earlier = (id_col == id_row) & (iota((ROWS, ROWS), 0) < iota((ROWS, ROWS), 1))
    rank = jnp.sum(earlier.astype(f32), axis=0, keepdims=True).astype(jnp.int32)
    group = id_int // PER
    within = (id_int % PER) * MOST + rank
    slot = away(group, x, zl) * SLOTS + within
    placed = (iota((GROUPS * SLOTS, ROWS), 0) == slot).astype(bf16)
    rows = jnp.dot(placed, q_ref[...], preferred_element_type=f32)
    tag_at = iota((8, ROWS), 0)
    tags = jnp.where(tag_at == 0, (iota((8, ROWS), 1) // TOP).astype(f32), 0.0)
    tags = jnp.where(tag_at == 1, gate_row, tags).astype(bf16)
    for g in range(GROUPS):
        here = (iota((ROWS, ROWS), 0) == slot - g * SLOTS).astype(bf16)
        info = lax.dot_general(tags, here, NT, preferred_element_type=f32)
        qsend_ref[g // 2, g % 2 * SLOTS : (g % 2 + 1) * SLOTS] = jnp.concatenate(
            [rows[g * SLOTS : g * SLOTS + PER * MOST], info], axis=0
        ).astype(bf16)
    slot = group * SLOTS + within
    slot_col = jnp.broadcast_to(slot.astype(f32), (ROWS, ROWS)).T.astype(jnp.int32)
    lane = iota((ROWS, ROWS), 1)
    back_ref[:, :ROWS] = (lane == slot_col).astype(bf16)
    back_ref[:, ROWS:] = (lane + ROWS == slot_col).astype(bf16)


def attend_half(at_ref, kv_ref, q_refs, s_ref, parity, best):
    n = GROUPS * SLOTS
    step = 4
    width = step * SPAN
    steps = CHIPS // step
    chunks = [
        q_refs[4][d // 2] if d % 2 else q_refs[d // 2][0:SLOTS] for d in range(GROUPS)
    ]
    queries = jnp.concatenate(chunks, axis=0)
    ctx = at_ref[0]
    tags = jnp.concatenate([chunk.astype(f32)[PER * MOST :] for chunk in chunks], axis=0)
    tags = jnp.concatenate([tags, tags], axis=0).T[0:SLOTS]
    token = jnp.concatenate([tags[:, g * 8 : g * 8 + 1] for g in range(GROUPS)], axis=0)
    gate = jnp.concatenate([tags[:, g * 8 + 1 : g * 8 + 2] for g in range(GROUPS)], axis=0)
    sources = [
        ((at_ref[2] - d // 2 + 4) % 4) * 2 + (at_ref[3] + d % 2) % 2 for d in range(GROUPS)
    ]
    source = jnp.concatenate([jnp.full((SLOTS, 1), d, jnp.int32) for d in sources], axis=0)
    pos = (source * (2 * CHIPS) + ctx) * TOK + token.astype(jnp.int32)
    scale = HD ** (-0.5) * math.log2(math.e)
    lane = iota((1, width), 1)

    def score(i, top):
        keys = kv_ref[pl.ds(i * step, step), 0:SPAN, :].reshape(width, HD)
        scores = lax.dot_general(queries, keys, NT, preferred_element_type=f32) * scale
        key_pos = (2 * (i * step + lane // SPAN) + parity) * SPAN + lane % SPAN
        scores = jnp.where(key_pos <= pos, scores, NEG_FLOOR)
        s_ref[i] = scores
        return jnp.maximum(top, jnp.maximum(scores[:, :HD], scores[:, HD:]))

    best = lax.fori_loop(0, steps, score, best, unroll=8)
    best = jnp.max(best, axis=1, keepdims=True)

    def weigh(i, carried):
        total, acc = carried
        scores = s_ref[i]
        exps = jnp.where(scores > 0.5 * NEG_FLOOR, jnp.exp2(scores - best), 0.0)
        values = kv_ref[pl.ds(i * step, step), SPAN : 2 * SPAN, :].reshape(width, HD)
        acc = acc + jnp.dot(exps.astype(bf16), values, preferred_element_type=f32)
        return total + exps[:, :HD] + exps[:, HD:], acc

    zero = jnp.zeros((n, HD), f32)
    total, acc = lax.fori_loop(0, steps, weigh, (zero, zero), unroll=8)
    return best, total, acc, gate, sources


def attend_own_kernel(at_ref, kv_ref, *refs):
    q_refs, (best_ref, total_ref, acc_ref, s_ref) = refs[:5], refs[5:]
    best = jnp.full((GROUPS * SLOTS, HD), NEG_FLOOR, f32)
    best, total, acc, _, _ = attend_half(at_ref, kv_ref, q_refs, s_ref, at_ref[1], best)
    best_ref[...] = jnp.broadcast_to(best, acc.shape)
    total_ref[...] = total
    acc_ref[...] = acc


def attend_kernel(at_ref, kv_ref, *refs):
    q_refs, (best_ref, total_ref, acc_ref, out_ref, s_ref) = refs[:5], refs[5:]
    before = best_ref[...]
    best, total, acc, gate, sources = attend_half(
        at_ref, kv_ref, q_refs, s_ref, 1 - at_ref[1], before
    )
    fade = jnp.exp2(before - best)
    total = jnp.sum(total + total_ref[...] * fade, axis=1, keepdims=True)
    acc = acc + acc_ref[...] * fade
    result = (gate * (acc / total)).astype(bf16)
    for d in range(GROUPS):
        out_ref[sources[d]] = result[d * SLOTS : (d + 1) * SLOTS]


def compact_kernel(back_ref, got_ref, out_ref):
    rows = jnp.dot(
        back_ref[...], got_ref[...].reshape(GROUPS * SLOTS, HD), preferred_element_type=f32
    ).astype(bf16)

    def fill(i, _):
        out_ref[i] = rows
        return 0

    lax.fori_loop(0, CHIPS, fill, 0)


def join_kernel(*refs):
    out_ref, sems = refs[4:]
    copies = [
        pltpu.make_async_copy(refs[k], out_ref.at[pl.ds(k * 2 * PER, 2 * PER)], sems.at[k])
        for k in range(4)
    ]
    for copy in copies:
        copy.start()
    for copy in copies:
        copy.wait()


def project_kernel(at_ref, rows_ref, kv_ref, *refs):
    mine_ref, other_ref, a_ref, w_ref, sems = refs[2:]
    copies = [pltpu.make_async_copy(refs[k], w_ref.at[k], sems.at[k]) for k in range(2)]
    for copy in copies:
        copy.start()
    x = at_ref[0]
    zl = at_ref[1]
    token = iota((1, ROWS), 1) // TOP
    target_at = iota((EXPERTS * TOK, ROWS), 0)

    def spread(i):
        ids = kv_ref[i, 2 * SPAN : KVROWS, :].astype(f32)[0:1].astype(jnp.int32)
        group = ids // PER
        piece = ((x - group // 2 + 4) % 4) * 2 + (group % 2 + zl) % 2
        target = (piece * PER + ids % PER) * TOK + token
        hot = (target_at == target).astype(bf16)
        got = jnp.dot(hot, rows_ref[i], preferred_element_type=f32)
        return got.reshape(EXPERTS, TOK, HD)

    def fill(i, _):
        both = jnp.concatenate([spread(2 * i), spread(2 * i + 1)], axis=1).astype(bf16)
        at = pl.ds(pl.multiple_of(i * 2 * TOK, 2 * TOK), 2 * TOK)
        for e in range(EXPERTS):
            a_ref[e // PER, at, (e % PER) * HD : (e % PER + 1) * HD] = both[e]
        return 0

    lax.fori_loop(0, CHIPS // 2, fill, 0, unroll=4)

    for copy in copies:
        copy.wait()
    total = jnp.zeros((CHIPS * TOK, 2 * HD), f32)
    for piece in range(GROUPS):
        part = slice(piece * PER, (piece + 1) * PER)
        near = w_ref[0, part].reshape(PER * HD, HD)
        far = w_ref[1, part].reshape(PER * HD, HD)
        weight = jnp.concatenate([near, far], axis=1)
        total = total + jnp.dot(a_ref[piece], weight, preferred_element_type=f32)
    mine_ref[...] = total[:, :HD].astype(bf16)
    other_ref[...] = total[:, HD:].astype(bf16)


SMEM = pl.BlockSpec(memory_space=pltpu.SMEM)
VMEM = pl.BlockSpec(memory_space=pltpu.VMEM)
ANY = pl.BlockSpec(memory_space=pl.ANY)
HBM = pl.BlockSpec(memory_space=pltpu.HBM)


def shifted(x, axis, count, by):
    return lax.ppermute(x, axis, [(i, (i + by) % count) for i in range(count)])


def run(queries, key_heads, value_heads, expert_ids, gate_logits, out_weight):
    zh, y, core = lax.axis_index("zh"), lax.axis_index("y"), lax.axis_index("core")
    x, zl = lax.axis_index("x"), lax.axis_index("zl")
    ctx = (zh * 8 + y) * 2 + core
    at = jnp.stack([ctx, core, x, zl]).astype(jnp.int32)
    at_exp = jnp.stack([x, zl, core]).astype(jnp.int32)
    shape = jax.ShapeDtypeStruct
    near = shifted(out_weight, "zl", 2, 1)
    kvsend = pl.pallas_call(
        prep_kv_kernel,
        in_specs=[VMEM] * 3,
        out_specs=HBM,
        out_shape=shape((CHIPS, KVROWS, HD), bf16),
        scratch_shapes=[pltpu.VMEM((KVROWS, HD), bf16), pltpu.SemaphoreType.DMA((CHIPS,))],
        name="prep_kv",
    )(key_heads.reshape(SPAN, HD), value_heads.reshape(SPAN, HD), expert_ids)
    kva = lax.all_to_all(kvsend, ("zh", "y"), 0, 0, tiled=True)
    back, qsend = pl.pallas_call(
        prep_q_kernel,
        in_specs=[VMEM] * 3,
        out_specs=[VMEM] * 2,
        out_shape=[
            shape((ROWS, GROUPS * SLOTS), bf16),
            shape((4, 2 * SLOTS, HD), bf16),
        ],
        name="prep_q",
    )(queries.reshape(ROWS, HD), expert_ids, gate_logits)
    qgot = [qsend[k] for k in range(4)]
    for k in range(1, 4):
        qgot[k] = shifted(qgot[k], "x", 4, k)
    crossing = jnp.stack([part[SLOTS:] for part in qgot])
    qgot.append(shifted(crossing, "zl", 2, 1))
    pair = jnp.concatenate([out_weight, near], axis=0)
    pieces = [pair]
    for k in range(1, 4):
        pieces.append(shifted(pair, "x", 4, k))
    near = pl.pallas_call(
        join_kernel,
        in_specs=[ANY] * 4,
        out_specs=ANY,
        out_shape=shape((EXPERTS, HD, HD), bf16),
        scratch_shapes=[pltpu.SemaphoreType.DMA((4,))],
        compiler_params=pltpu.CompilerParams(vmem_limit_bytes=4 << 20),
        name="join",
    )(*pieces)
    far = shifted(near, "core", 2, 1)
    kvb = shifted(kva, "core", 2, 1)
    state = shape((GROUPS * SLOTS, HD), f32)
    scratch = [pltpu.VMEM((8, GROUPS * SLOTS, 4 * SPAN), f32)]
    running = pl.pallas_call(
        attend_own_kernel,
        in_specs=[SMEM] + [VMEM] * 6,
        out_specs=[VMEM] * 3,
        out_shape=[state] * 3,
        scratch_shapes=scratch,
        compiler_params=pltpu.CompilerParams(vmem_limit_bytes=14 << 20),
        name="attend_own",
    )(at, kva, *qgot)
    attended = pl.pallas_call(
        attend_kernel,
        in_specs=[SMEM] + [VMEM] * 9,
        out_specs=VMEM,
        out_shape=shape((GROUPS, SLOTS, HD), bf16),
        scratch_shapes=scratch,
        compiler_params=pltpu.CompilerParams(vmem_limit_bytes=14 << 20),
        name="attend",
    )(at, kvb, *qgot, *running)
    home = lax.all_to_all(attended, ("x", "zl"), 0, 0, tiled=True)
    rows = pl.pallas_call(
        compact_kernel,
        in_specs=[VMEM, VMEM],
        out_specs=VMEM,
        out_shape=shape((CHIPS, ROWS, HD), bf16),
        compiler_params=pltpu.CompilerParams(vmem_limit_bytes=8 << 20),
        name="compact",
    )(back, home)
    rows = lax.all_to_all(rows, ("zh", "y"), 0, 0, tiled=True)
    mine, other = pl.pallas_call(
        project_kernel,
        in_specs=[SMEM] + [VMEM] * 2 + [HBM] * 2,
        out_specs=[VMEM, VMEM],
        out_shape=[shape((CHIPS * TOK, HD), bf16)] * 2,
        scratch_shapes=[
            pltpu.VMEM((GROUPS, CHIPS * TOK, PER * HD), bf16),
            pltpu.VMEM((2, EXPERTS, HD, HD), bf16),
            pltpu.SemaphoreType.DMA((2,)),
        ],
        compiler_params=pltpu.CompilerParams(vmem_limit_bytes=48 << 20),
        name="project",
    )(at_exp, rows, kva, near, far)
    got = shifted(other, "core", 2, 1)
    own = lax.broadcasted_iota(jnp.int32, (CHIPS, 2, TOK, HD), 1) == core
    mine = mine.reshape(CHIPS, 1, TOK, HD)
    got = got.reshape(CHIPS, 1, TOK, HD)
    return jnp.where(own, mine, got).reshape(2 * CHIPS * TOK, HD)


def solution(mesh):
    fine = Mesh(mesh.devices.reshape(4, 8, 2, 4, 2), ("zh", "y", "core", "x", "zl"))
    ctx, exp = ("zh", "y", "core"), ("x", "zl")
    in_specs = (
        P(exp + ctx, None, None),
        P(ctx, exp, None),
        P(ctx, exp, None),
        P(exp + ctx, None),
        P(exp + ctx, None),
        P(exp, None, ctx),
    )
    return jax.shard_map(run, mesh=fine, in_specs=in_specs, out_specs=P(exp, ctx), check_vma=False)
```

```python
import math

import jax
import jax.numpy as jnp
from jax import lax
from jax.experimental import pallas as pl
from jax.experimental.pallas import tpu as pltpu
from jax.sharding import Mesh, PartitionSpec as P


EXPERTS = 64
HD = 128
TOP = 16
MOST = 3
TOK = 8
ROWS = TOK * TOP
GROUPS = 8
PER = EXPERTS // GROUPS
SLOTS = 32
SPAN = 64
CHIPS = 32
KVROWS = 2 * SPAN + 8
NEG_FLOOR = -1e30


f32 = jnp.float32
bf16 = jnp.bfloat16
NT = (((1,), (1,)), ((), ()))


def iota(shape, dim):
    return lax.broadcasted_iota(jnp.int32, shape, dim)


def away(group, x, zl):
    return ((group // 2 - x + 4) % 4) * 2 + (group % 2 + zl) % 2


def prep_kernel(
    q_ref, k_ref, v_ref, ids_ref, logit_ref, w_ref,
    kvsend_ref, back_ref, qnear_ref, cargo_ref, chunk_ref, sems,
):
    x = lax.axis_index("x")
    zl = lax.axis_index("zl")
    spread = (iota((TOP, ROWS), 1) % TOP == iota((TOP, ROWS), 0)).astype(bf16)
    own = iota((TOK, ROWS), 1) // TOP == iota((TOK, ROWS), 0)

    def as_row(table):
        wide = jnp.dot(table.astype(bf16), spread, preferred_element_type=f32)
        return jnp.sum(jnp.where(own, wide, 0.0), axis=0, keepdims=True)

    id_row = as_row(ids_ref[...].astype(f32))
    chunk_ref[0:SPAN] = k_ref[...]
    chunk_ref[SPAN : 2 * SPAN] = v_ref[...]
    chunk_ref[2 * SPAN : KVROWS] = jnp.broadcast_to(id_row, (8, ROWS)).astype(bf16)
    copies = [
        pltpu.make_async_copy(chunk_ref, kvsend_ref.at[i], sems.at[i]) for i in range(CHIPS)
    ]
    for copy in copies:
        copy.start()
    gate_exp = jnp.exp(logit_ref[...])
    gate_row = as_row(gate_exp / jnp.sum(gate_exp, axis=1, keepdims=True))
    id_int = id_row.astype(jnp.int32)
    id_col = jnp.broadcast_to(id_row, (ROWS, ROWS)).T
    earlier = (id_col == id_row) & (iota((ROWS, ROWS), 0) < iota((ROWS, ROWS), 1))
    rank = jnp.sum(earlier.astype(f32), axis=0, keepdims=True).astype(jnp.int32)
    group = id_int // PER
    within = (id_int % PER) * MOST + rank
    slot = away(group, x, zl) * SLOTS + within
    placed = (iota((GROUPS * SLOTS, ROWS), 0) == slot).astype(bf16)
    rows = jnp.dot(placed, q_ref[...], preferred_element_type=f32)
    tag_at = iota((8, ROWS), 0)
    tags = jnp.where(tag_at == 0, (iota((8, ROWS), 1) // TOP).astype(f32), 0.0)
    tags = jnp.where(tag_at == 1, gate_row, tags).astype(bf16)
    for g in range(GROUPS):
        here = (iota((ROWS, ROWS), 0) == slot - g * SLOTS).astype(bf16)
        info = lax.dot_general(tags, here, NT, preferred_element_type=f32)
        chunk = jnp.concatenate(
            [rows[g * SLOTS : g * SLOTS + PER * MOST], info], axis=0
        ).astype(bf16)
        if g % 2 == 0:
            qnear_ref[g // 2] = chunk
        else:
            cargo_ref[PER * HD + g // 2 * SLOTS : PER * HD + (g // 2 + 1) * SLOTS] = chunk
    cargo_ref[0 : PER * HD] = w_ref[...].reshape(PER * HD, HD)
    slot = group * SLOTS + within
    slot_col = jnp.broadcast_to(slot.astype(f32), (ROWS, ROWS)).T.astype(jnp.int32)
    lane = iota((ROWS, ROWS), 1)
    back_ref[:, :ROWS] = (lane == slot_col).astype(bf16)
    back_ref[:, ROWS:] = (lane + ROWS == slot_col).astype(bf16)
    for copy in copies:
        copy.wait()


def attend_half(at_ref, kv_ref, q_refs, s_ref, parity, best):
    n = GROUPS * SLOTS
    step = 4
    width = step * SPAN
    steps = CHIPS // step
    chunks = [
        q_refs[d // 2][d % 2 * SLOTS : (d % 2 + 1) * SLOTS] for d in range(GROUPS)
    ]
    queries = jnp.concatenate(chunks, axis=0)
    ctx = at_ref[0]
    tags = jnp.concatenate([chunk.astype(f32)[PER * MOST :] for chunk in chunks], axis=0)
    tags = jnp.concatenate([tags, tags], axis=0).T[0:SLOTS]
    token = jnp.concatenate([tags[:, g * 8 : g * 8 + 1] for g in range(GROUPS)], axis=0)
    gate = jnp.concatenate([tags[:, g * 8 + 1 : g * 8 + 2] for g in range(GROUPS)], axis=0)
    sources = [
        ((at_ref[2] - d // 2 + 4) % 4) * 2 + (at_ref[3] + d % 2) % 2 for d in range(GROUPS)
    ]
    source = jnp.concatenate([jnp.full((SLOTS, 1), d, jnp.int32) for d in sources], axis=0)
    pos = (source * (2 * CHIPS) + ctx) * TOK + token.astype(jnp.int32)
    scale = HD ** (-0.5) * math.log2(math.e)
    lane = iota((1, width), 1)

    def score(i, top):
        keys = kv_ref[pl.ds(i * step, step), 0:SPAN, :].reshape(width, HD)
        scores = lax.dot_general(queries, keys, NT, preferred_element_type=f32) * scale
        key_pos = (2 * (i * step + lane // SPAN) + parity) * SPAN + lane % SPAN
        scores = jnp.where(key_pos <= pos, scores, NEG_FLOOR)
        s_ref[i] = scores
        return jnp.maximum(top, jnp.maximum(scores[:, :HD], scores[:, HD:]))

    best = lax.fori_loop(0, steps, score, best, unroll=8)
    best = jnp.max(best, axis=1, keepdims=True)

    def weigh(i, carried):
        total, acc = carried
        scores = s_ref[i]
        exps = jnp.where(scores > 0.5 * NEG_FLOOR, jnp.exp2(scores - best), 0.0)
        values = kv_ref[pl.ds(i * step, step), SPAN : 2 * SPAN, :].reshape(width, HD)
        acc = acc + jnp.dot(exps.astype(bf16), values, preferred_element_type=f32)
        return total + exps[:, :HD] + exps[:, HD:], acc

    zero = jnp.zeros((n, HD), f32)
    total, acc = lax.fori_loop(0, steps, weigh, (zero, zero), unroll=8)
    return best, total, acc, gate, sources


def attend_own_kernel(at_ref, kv_ref, *refs):
    q_refs, (best_ref, total_ref, acc_ref, s_ref) = refs[:4], refs[4:]
    best = jnp.full((GROUPS * SLOTS, HD), NEG_FLOOR, f32)
    best, total, acc, _, _ = attend_half(at_ref, kv_ref, q_refs, s_ref, at_ref[1], best)
    best_ref[...] = jnp.broadcast_to(best, acc.shape)
    total_ref[...] = total
    acc_ref[...] = acc


def attend_kernel(at_ref, kv_ref, *refs):
    q_refs, (best_ref, total_ref, acc_ref, out_ref, s_ref) = refs[:4], refs[4:]
    before = best_ref[...]
    best, total, acc, gate, sources = attend_half(
        at_ref, kv_ref, q_refs, s_ref, 1 - at_ref[1], before
    )
    fade = jnp.exp2(before - best)
    total = jnp.sum(total + total_ref[...] * fade, axis=1, keepdims=True)
    acc = acc + acc_ref[...] * fade
    result = (gate * (acc / total)).astype(bf16)
    for d in range(GROUPS):
        out_ref[sources[d]] = result[d * SLOTS : (d + 1) * SLOTS]


def compact_kernel(back_ref, got_ref, out_ref, rows_ref, sems):
    rows_ref[...] = jnp.dot(
        back_ref[...], got_ref[...].reshape(GROUPS * SLOTS, HD), preferred_element_type=f32
    ).astype(bf16)
    copies = [pltpu.make_async_copy(rows_ref, out_ref.at[i], sems.at[i]) for i in range(CHIPS)]
    for copy in copies:
        copy.start()
    for copy in copies:
        copy.wait()


def join_kernel(*refs):
    out_ref, sems = refs[4:]
    copies = [
        pltpu.make_async_copy(refs[k], out_ref.at[pl.ds(k * 2 * PER, 2 * PER)], sems.at[k])
        for k in range(4)
    ]
    for copy in copies:
        copy.start()
    for copy in copies:
        copy.wait()


def project_kernel(at_ref, rows_ref, kv_ref, *refs):
    mine_ref, other_ref, a_ref, w_ref, sems = refs[2:]
    copies = [pltpu.make_async_copy(refs[k], w_ref.at[k], sems.at[k]) for k in range(2)]
    for copy in copies:
        copy.start()
    x = at_ref[0]
    zl = at_ref[1]
    token = iota((1, ROWS), 1) // TOP
    target_at = iota((EXPERTS * TOK, ROWS), 0)

    def spread(i):
        ids = kv_ref[i, 2 * SPAN : KVROWS, :].astype(f32)[0:1].astype(jnp.int32)
        group = ids // PER
        piece = ((x - group // 2 + 4) % 4) * 2 + (group % 2 + zl) % 2
        target = (piece * PER + ids % PER) * TOK + token
        hot = (target_at == target).astype(bf16)
        got = jnp.dot(hot, rows_ref[i], preferred_element_type=f32)
        return got.reshape(EXPERTS, TOK, HD)

    def fill(i, _):
        both = jnp.concatenate([spread(2 * i), spread(2 * i + 1)], axis=1).astype(bf16)
        at = pl.ds(pl.multiple_of(i * 2 * TOK, 2 * TOK), 2 * TOK)
        for e in range(EXPERTS):
            a_ref[e // PER, at, (e % PER) * HD : (e % PER + 1) * HD] = both[e]
        return 0

    lax.fori_loop(0, CHIPS // 2, fill, 0, unroll=4)

    for copy in copies:
        copy.wait()
    total = jnp.zeros((CHIPS * TOK, 2 * HD), f32)
    for piece in range(GROUPS):
        part = slice(piece * PER, (piece + 1) * PER)
        near = w_ref[0, part].reshape(PER * HD, HD)
        far = w_ref[1, part].reshape(PER * HD, HD)
        weight = jnp.concatenate([near, far], axis=1)
        total = total + jnp.dot(a_ref[piece], weight, preferred_element_type=f32)
    mine_ref[...] = total[:, :HD].astype(bf16)
    other_ref[...] = total[:, HD:].astype(bf16)


SMEM = pl.BlockSpec(memory_space=pltpu.SMEM)
VMEM = pl.BlockSpec(memory_space=pltpu.VMEM)
ANY = pl.BlockSpec(memory_space=pl.ANY)
HBM = pl.BlockSpec(memory_space=pltpu.HBM)


def shifted(x, axis, count, by):
    return lax.ppermute(x, axis, [(i, (i + by) % count) for i in range(count)])


def run(queries, key_heads, value_heads, expert_ids, gate_logits, out_weight):
    zh, y, core = lax.axis_index("zh"), lax.axis_index("y"), lax.axis_index("core")
    x, zl = lax.axis_index("x"), lax.axis_index("zl")
    ctx = (zh * 8 + y) * 2 + core
    at = jnp.stack([ctx, core, x, zl]).astype(jnp.int32)
    at_exp = jnp.stack([x, zl, core]).astype(jnp.int32)
    shape = jax.ShapeDtypeStruct
    kvsend, back, qnear, cargo = pl.pallas_call(
        prep_kernel,
        in_specs=[VMEM] * 6,
        out_specs=[HBM] + [VMEM] * 3,
        scratch_shapes=[pltpu.VMEM((KVROWS, HD), bf16), pltpu.SemaphoreType.DMA((CHIPS,))],
        out_shape=[
            shape((CHIPS, KVROWS, HD), bf16),
            shape((ROWS, GROUPS * SLOTS), bf16),
            shape((4, SLOTS, HD), bf16),
            shape((PER * HD + 4 * SLOTS, HD), bf16),
        ],
        name="prep",
    )(
        queries.reshape(ROWS, HD),
        key_heads.reshape(SPAN, HD),
        value_heads.reshape(SPAN, HD),
        expert_ids,
        gate_logits,
        out_weight,
    )
    kva = lax.all_to_all(kvsend, ("zh", "y"), 0, 0, tiled=True)
    got = shifted(cargo, "zl", 2, 1)
    crossed = got[PER * HD :].reshape(4, SLOTS, HD)
    qpair = jnp.concatenate([qnear, crossed], axis=1)
    qgot = [qpair[k] for k in range(4)]
    for k in range(1, 4):
        qgot[k] = shifted(qgot[k], "x", 4, k)
    pair = jnp.concatenate([out_weight, got[: PER * HD].reshape(PER, HD, HD)], axis=0)
    pieces = [pair]
    for k in range(1, 4):
        pieces.append(shifted(pair, "x", 4, k))
    near = pl.pallas_call(
        join_kernel,
        in_specs=[ANY] * 4,
        out_specs=ANY,
        out_shape=shape((EXPERTS, HD, HD), bf16),
        scratch_shapes=[pltpu.SemaphoreType.DMA((4,))],
        compiler_params=pltpu.CompilerParams(vmem_limit_bytes=4 << 20),
        name="join",
    )(*pieces)
    far = shifted(near, "core", 2, 1)
    kvb = shifted(kva, "core", 2, 1)
    state = shape((GROUPS * SLOTS, HD), f32)
    scratch = [pltpu.VMEM((8, GROUPS * SLOTS, 4 * SPAN), f32)]
    running = pl.pallas_call(
        attend_own_kernel,
        in_specs=[SMEM] + [VMEM] * 5,
        out_specs=[VMEM] * 3,
        out_shape=[state] * 3,
        scratch_shapes=scratch,
        compiler_params=pltpu.CompilerParams(vmem_limit_bytes=14 << 20),
        name="attend_own",
    )(at, kva, *qgot)
    attended = pl.pallas_call(
        attend_kernel,
        in_specs=[SMEM] + [VMEM] * 8,
        out_specs=VMEM,
        out_shape=shape((GROUPS, SLOTS, HD), bf16),
        scratch_shapes=scratch,
        compiler_params=pltpu.CompilerParams(vmem_limit_bytes=14 << 20),
        name="attend",
    )(at, kvb, *qgot, *running)
    home = lax.all_to_all(attended, ("x", "zl"), 0, 0, tiled=True)
    rows = pl.pallas_call(
        compact_kernel,
        in_specs=[VMEM, VMEM],
        out_specs=HBM,
        out_shape=shape((CHIPS, ROWS, HD), bf16),
        scratch_shapes=[pltpu.VMEM((ROWS, HD), bf16), pltpu.SemaphoreType.DMA((CHIPS,))],
        compiler_params=pltpu.CompilerParams(vmem_limit_bytes=8 << 20),
        name="compact",
    )(back, home)
    rows = lax.all_to_all(rows, ("zh", "y"), 0, 0, tiled=True)
    mine, other = pl.pallas_call(
        project_kernel,
        in_specs=[SMEM] + [VMEM] * 2 + [HBM] * 2,
        out_specs=[VMEM, VMEM],
        out_shape=[shape((CHIPS * TOK, HD), bf16)] * 2,
        scratch_shapes=[
            pltpu.VMEM((GROUPS, CHIPS * TOK, PER * HD), bf16),
            pltpu.VMEM((2, EXPERTS, HD, HD), bf16),
            pltpu.SemaphoreType.DMA((2,)),
        ],
        compiler_params=pltpu.CompilerParams(vmem_limit_bytes=48 << 20),
        name="project",
    )(at_exp, rows, kva, near, far)
    got = shifted(other, "core", 2, 1)
    own = lax.broadcasted_iota(jnp.int32, (CHIPS, 2, TOK, HD), 1) == core
    mine = mine.reshape(CHIPS, 1, TOK, HD)
    got = got.reshape(CHIPS, 1, TOK, HD)
    return jnp.where(own, mine, got).reshape(2 * CHIPS * TOK, HD)


def solution(mesh):
    fine = Mesh(mesh.devices.reshape(4, 8, 2, 4, 2), ("zh", "y", "core", "x", "zl"))
    ctx, exp = ("zh", "y", "core"), ("x", "zl")
    in_specs = (
        P(exp + ctx, None, None),
        P(ctx, exp, None),
        P(ctx, exp, None),
        P(exp + ctx, None),
        P(exp + ctx, None),
        P(exp, None, ctx),
    )
    return jax.shard_map(run, mesh=fine, in_specs=in_specs, out_specs=P(exp, ctx), check_vma=False)
```
